32 devices in a mesh: dap: 16 (over z, y, x), dp: 2 (over core).
Axes of the slice: x: 2, y: 2, z: 4, core: 2. Of those that a mesh axis runs over, the one named last changes fastest.
Arguments:
- edge_embedding: bfloat16 [192, 96, 128], P(('dp', 'dap')), parts along dimension 0, may hold values from -6 to 6
- alignment_embedding: bfloat16 [128, 96, 256], P('dp', 'dap'), parts along dimension 0, may hold values from -6 to 6
- tensor_flank_matrix: bfloat16 [256, 64], replicated, may hold values from -0.375 to 0.375
- tensor_final_matrix: bfloat16 [1024, 128], replicated, may hold values from -0.75 to 0.75
- outward_sigmoid_matrix: bfloat16 [128, 640], replicated, may hold values from -0.5 to 0.5
- outward_final_matrix: bfloat16 [128, 128], replicated, may hold values from -0.5 to 0.5
- inward_sigmoid_matrix: bfloat16 [128, 640], replicated, may hold values from -0.5 to 0.5
- inward_final_matrix: bfloat16 [128, 128], replicated, may hold values from -0.5 to 0.5
- adjoint_seed: bfloat16 [192, 96, 128], P(('dp', 'dap')), parts along dimension 0, may hold values from -6 to 6
Outputs:
- edge_embedding_updated: bfloat16 [192, 96, 128], P(('dp', 'dap')), parts along dimension 0
- edge_embedding_adjoint: bfloat16 [192, 96, 128], P(('dp', 'dap')), parts along dimension 0
- alignment_adjoint: bfloat16 [128, 96, 256], P('dp', 'dap'), parts along dimension 0
- outer_proj_grad: float32 [512, 64], P('dp'), parts along dimension 0
- outer_final_grad: float32 [2048, 128], P('dp'), parts along dimension 0
- outgoing_proj_grad: float32 [256, 640], P('dp'), parts along dimension 0
- outgoing_final_grad: float32 [256, 128], P('dp'), parts along dimension 0
- incoming_proj_grad: float32 [256, 640], P('dp'), parts along dimension 0
- incoming_final_grad: float32 [256, 128], P('dp'), parts along dimension 0
The draws below stay inside these ranges and needn't reach their ends.
There are 2 independent parts, one for each index of `dp`. The reference program is written for one: setup_inputs(seed, part) draws one part's arguments, and reference() takes and returns one part's arrays. A program takes and returns all parts, laid end to end along the dimension named above; an argument that names none is the same for every part. Nothing has to cross between parts.
All inputs are finite; a program needn't handle non-finite values.
Results may differ from the reference program's by a relative error of at most 0.02.
Values may be sent and summed in bfloat16 or wider, within the bound.
No kernel may reach another device: no remote copies, remote signals or barrier semaphores. Data moves between devices by JAX's collectives and lax.ppermute only.
A program may use at most 128 MiB of HBM per device.

```python
import jax
import jax.numpy as jnp
from jax import lax

ALIGN_FEATURES = 256
EDGE_FEATURES = 128
CH = 128
HIDDEN_WIDTH = 32
ALIGN_ROWS = 64
AMINO_TOTAL = 96


def strengthened(array, rng, source, target, blocks, factor):
    def block_of(axis_at):
        return (jnp.arange(array.shape[axis_at]) // (array.shape[axis_at] // blocks)).reshape((-1,) + (1,) * (array.ndim - 1 - axis_at))

    one_side = jax.random.permutation(rng, blocks)[block_of(target)]
    second = (block_of(target) + blocks // 2) % blocks
    return jnp.where((block_of(source) == one_side) | (block_of(source) == second), factor * array, array)


def block_levels(rng, dims, cuts, low, largest):
    def one(dim, parts):
        draws = jax.random.uniform(jax.random.fold_in(jax.random.fold_in(rng, 6), dim), (parts,), jnp.float32, low / len(cuts), largest / len(cuts))
        return jnp.repeat(jnp.exp(draws), dims[dim] // parts).reshape((-1,) + (1,) * (len(dims) - dim - 1))

    loudness = one(*cuts[0])
    for cut in cuts[1:]:
        loudness = loudness * one(*cut)
    return loudness


def scatter_about(stream_key, dims, spread, bound, shards=(), dtype=jnp.bfloat16):
    factor_of = block_levels(stream_key, dims, shards, -0.22, 0.18) if shards else 1.0
    drawn = jax.random.normal(stream_key, dims, jnp.float32) * spread * factor_of
    return jnp.minimum(jnp.maximum(drawn, -bound), bound).astype(dtype)


def gaussian_with(key, dims, width, bound, split, heavy, dtype=jnp.bfloat16):
    entries = width * jax.random.normal(key, dims, jnp.float32)
    if split:
        entries = entries * block_levels(key, dims, split, -0.22, 0.18)
    return jnp.clip(strengthened(entries, jax.random.fold_in(key, 3), *heavy), -bound, bound).astype(dtype)


def setup_inputs(seed: int = 0, part: int = 0) -> dict:
    seeds = jax.random.split(jax.random.key(seed), 10)
    part_splits = jax.random.split(jax.random.fold_in(seeds[9], part), 10)
    edge_embedding = scatter_about(part_splits[0], (AMINO_TOTAL, AMINO_TOTAL, EDGE_FEATURES), 1.0, 6.0, ((0, 16),))
    alignment_embedding = scatter_about(part_splits[1], (ALIGN_ROWS, AMINO_TOTAL, ALIGN_FEATURES), 1.0, 6.0, ((1, 16),))
    tensor_flank_matrix = scatter_about(seeds[2], (ALIGN_FEATURES, 2 * HIDDEN_WIDTH), ALIGN_FEATURES ** -0.5, 0.375)
    tensor_final_matrix = scatter_about(seeds[3], (HIDDEN_WIDTH * HIDDEN_WIDTH, EDGE_FEATURES), (HIDDEN_WIDTH * HIDDEN_WIDTH // 16) ** -0.5, 0.75)
    outward_sigmoid_matrix = scatter_about(seeds[4], (EDGE_FEATURES, 4 * CH + EDGE_FEATURES), EDGE_FEATURES ** -0.5, 0.5)
    outward_final_matrix = scatter_about(seeds[5], (CH, EDGE_FEATURES), CH ** -0.5, 0.5)
    inward_sigmoid_matrix = scatter_about(seeds[6], (EDGE_FEATURES, 4 * CH + EDGE_FEATURES), EDGE_FEATURES ** -0.5, 0.5)
    inward_final_matrix = scatter_about(seeds[7], (CH, EDGE_FEATURES), CH ** -0.5, 0.5)
    adjoint_seed = gaussian_with(part_splits[8], (AMINO_TOTAL, AMINO_TOTAL, EDGE_FEATURES), 1.0, 6.0, ((0, 16),), (0, 1, 16, 2.0))
    return dict(edge_embedding=edge_embedding, alignment_embedding=alignment_embedding, tensor_flank_matrix=tensor_flank_matrix, tensor_final_matrix=tensor_final_matrix, outward_sigmoid_matrix=outward_sigmoid_matrix, outward_final_matrix=outward_final_matrix, inward_sigmoid_matrix=inward_sigmoid_matrix, inward_final_matrix=inward_final_matrix, adjoint_seed=adjoint_seed)


EPSILON = 1e-05

def truncated_numbers(values):
    return lax.optimization_barrier(values.astype(jnp.bfloat16))

def edge_standardized(values, which_axis):
    average = lax.optimization_barrier(jnp.mean(values, axis=which_axis, keepdims=True))
    centred = values - average
    factor = lax.rsqrt(lax.optimization_barrier(jnp.mean(centred * centred, axis=which_axis, keepdims=True)) + EPSILON)
    return centred * factor

def standardizer_adjoint(values, gradient, which_axis):
    average = lax.optimization_barrier(jnp.mean(values, axis=which_axis, keepdims=True))
    centred = values - average
    factor = lax.rsqrt(lax.optimization_barrier(jnp.mean(centred * centred, axis=which_axis, keepdims=True)) + EPSILON)
    hatted = centred * factor
    return factor * (gradient - lax.optimization_barrier(jnp.mean(gradient, axis=which_axis, keepdims=True)) - hatted * lax.optimization_barrier(jnp.mean(gradient * hatted, axis=which_axis, keepdims=True)))

def sigmoid_pieces(edge_entry, linear_mapping, latent_tensor):
    standardized_edges = truncated_numbers(edge_standardized(edge_entry.astype(jnp.float32), -1))
    alignment_mapped = jnp.dot(standardized_edges, linear_mapping, preferred_element_type=jnp.float32)
    source_masked = truncated_numbers(jax.nn.sigmoid(alignment_mapped[..., :latent_tensor]) * alignment_mapped[..., latent_tensor:2 * latent_tensor])
    target_masked = truncated_numbers(jax.nn.sigmoid(alignment_mapped[..., 2 * latent_tensor:3 * latent_tensor]) * alignment_mapped[..., 3 * latent_tensor:4 * latent_tensor])
    sigmoid_factor = jax.nn.sigmoid(alignment_mapped[..., 4 * latent_tensor:])
    return (standardized_edges, alignment_mapped, source_masked, target_masked, sigmoid_factor)

def contract(source_masked, target_masked, outgoing):
    left_wide = source_masked.astype(jnp.float32)
    target_broad = target_masked.astype(jnp.float32)
    if outgoing:
        triangle_contraction = jnp.einsum('ikc,jkc->ijc', left_wide, target_broad)
    else:
        triangle_contraction = jnp.einsum('kic,kjc->ijc', left_wide, target_broad)
    return truncated_numbers(triangle_contraction)

def triangle_update(edge_entry, linear_mapping, final, outgoing):
    latent_tensor = final.shape[0]
    standardized_edges, alignment_mapped, source_masked, target_masked, sigmoid_factor = sigmoid_pieces(edge_entry, linear_mapping, latent_tensor)
    triangle = contract(source_masked, target_masked, outgoing)
    unit_norm = truncated_numbers(edge_standardized(triangle.astype(jnp.float32), -1))
    values = jnp.dot(unit_norm, final, preferred_element_type=jnp.float32)
    return truncated_numbers(edge_entry.astype(jnp.float32) + sigmoid_factor * values)

def triangle_back(edge_entry, linear_mapping, final, outgoing, gradient):
    latent_tensor = final.shape[0]
    standardized_edges, alignment_mapped, source_masked, target_masked, sigmoid_factor = sigmoid_pieces(edge_entry, linear_mapping, latent_tensor)
    triangle = contract(source_masked, target_masked, outgoing)
    tri_wide = triangle.astype(jnp.float32)
    unit_norm = truncated_numbers(edge_standardized(tri_wide, -1))
    values = jnp.dot(unit_norm, final, preferred_element_type=jnp.float32)
    scaled = truncated_numbers(gradient * sigmoid_factor)
    final_sum = jnp.einsum('ijc,ijz->cz', unit_norm.astype(jnp.float32), scaled.astype(jnp.float32))
    grad_unit = jnp.dot(scaled, final.T, preferred_element_type=jnp.float32)
    adjoint_sigmoid = gradient * values * sigmoid_factor * (1.0 - sigmoid_factor)
    grad_triangle = truncated_numbers(standardizer_adjoint(tri_wide, grad_unit, -1)).astype(jnp.float32)
    left_wide = source_masked.astype(jnp.float32)
    target_broad = target_masked.astype(jnp.float32)
    if outgoing:
        source_adjoint = jnp.einsum('ijc,jkc->ikc', grad_triangle, target_broad)
        target_adjoint = jnp.einsum('ijc,ikc->jkc', grad_triangle, left_wide)
    else:
        source_adjoint = jnp.einsum('ijc,kjc->kic', grad_triangle, target_broad)
        target_adjoint = jnp.einsum('ijc,kic->kjc', grad_triangle, left_wide)
    source_adjoint = truncated_numbers(source_adjoint).astype(jnp.float32)
    target_adjoint = truncated_numbers(target_adjoint).astype(jnp.float32)
    logistic_primary = jax.nn.sigmoid(alignment_mapped[..., :latent_tensor])
    logistic_tertiary = jax.nn.sigmoid(alignment_mapped[..., 2 * latent_tensor:3 * latent_tensor])
    adjoint_linear_input = truncated_numbers(jnp.concatenate([source_adjoint * alignment_mapped[..., latent_tensor:2 * latent_tensor] * logistic_primary * (1.0 - logistic_primary), source_adjoint * logistic_primary, target_adjoint * alignment_mapped[..., 3 * latent_tensor:4 * latent_tensor] * logistic_tertiary * (1.0 - logistic_tertiary), target_adjoint * logistic_tertiary, adjoint_sigmoid], axis=-1))
    proj_sum = jnp.einsum('ijz,ijc->zc', standardized_edges.astype(jnp.float32), adjoint_linear_input.astype(jnp.float32))
    grad_norm = jnp.dot(adjoint_linear_input, linear_mapping.T, preferred_element_type=jnp.float32)
    grad_pair = gradient + standardizer_adjoint(edge_entry.astype(jnp.float32), grad_norm, -1)
    return (grad_pair, proj_sum, final_sum)

def reference(edge_embedding, alignment_embedding, tensor_flank_matrix, tensor_final_matrix, outward_sigmoid_matrix, outward_final_matrix, inward_sigmoid_matrix, inward_final_matrix, adjoint_seed):
    alignment_standardized = truncated_numbers(edge_standardized(alignment_embedding.astype(jnp.float32), -1))
    alignment_mapped = jnp.dot(alignment_standardized, tensor_flank_matrix, preferred_element_type=jnp.float32)
    tensor_source_factor = truncated_numbers(alignment_mapped[..., :HIDDEN_WIDTH])
    tensor_target_factor = truncated_numbers(alignment_mapped[..., HIDDEN_WIDTH:])
    tile_lines = 64 if AMINO_TOTAL % 64 == 0 else AMINO_TOTAL
    tile_number = AMINO_TOTAL // tile_lines
    source_tiles = jnp.transpose(tensor_source_factor.reshape(ALIGN_ROWS, tile_number, tile_lines, HIDDEN_WIDTH), (1, 0, 2, 3))
    pair_blocks = edge_embedding.reshape(tile_number, tile_lines, AMINO_TOTAL, EDGE_FEATURES)
    target_broad = tensor_target_factor.astype(jnp.float32)

    def outer_rows(source_lines):
        triangle_contraction = jnp.einsum('sic,sjd->ijcd', source_lines.astype(jnp.float32), target_broad)
        return truncated_numbers(triangle_contraction.reshape(tile_lines, AMINO_TOTAL, HIDDEN_WIDTH * HIDDEN_WIDTH) / ALIGN_ROWS)

    def forward_block(pieces):
        source_lines, pair_rows = pieces
        update = jnp.dot(outer_rows(source_lines), tensor_final_matrix, preferred_element_type=jnp.float32)
        return truncated_numbers(pair_rows.astype(jnp.float32) + update)
    pair_one = lax.map(forward_block, (source_tiles, pair_blocks)).reshape(AMINO_TOTAL, AMINO_TOTAL, EDGE_FEATURES)
    pair_two = triangle_update(pair_one, outward_sigmoid_matrix, outward_final_matrix, True)
    edge_embedding_updated = triangle_update(pair_two, inward_sigmoid_matrix, inward_final_matrix, False)
    grad_two, inward_sigmoid_accrual, inward_final_accrual = triangle_back(pair_two, inward_sigmoid_matrix, inward_final_matrix, False, adjoint_seed.astype(jnp.float32))
    grad_one, outward_sigmoid_accrual, outward_final_accrual = triangle_back(pair_one, outward_sigmoid_matrix, outward_final_matrix, True, grad_two)
    edge_embedding_adjoint = truncated_numbers(grad_one)
    grad_blocks = edge_embedding_adjoint.reshape(tile_number, tile_lines, AMINO_TOTAL, EDGE_FEATURES)

    def backward_block(running, pieces):
        final_sum, target_accrual = running
        source_lines, grad_rows = pieces
        outer_block = outer_rows(source_lines)
        final_sum = final_sum + jnp.einsum('ijk,ijz->kz', outer_block.astype(jnp.float32), grad_rows.astype(jnp.float32))
        adjoint_tensor_mean = truncated_numbers(jnp.dot(grad_rows, tensor_final_matrix.T, preferred_element_type=jnp.float32))
        adjoint_tensor_mean = adjoint_tensor_mean.astype(jnp.float32).reshape(tile_lines, AMINO_TOTAL, HIDDEN_WIDTH, HIDDEN_WIDTH)
        source_piece = jnp.einsum('mopz,loz->lmp', adjoint_tensor_mean, target_broad) / ALIGN_ROWS
        target_accrual = target_accrual + jnp.einsum('gxqp,vgq->vxp', adjoint_tensor_mean, source_lines.astype(jnp.float32)) / ALIGN_ROWS
        return ((final_sum, target_accrual), source_piece)
    starting_tensor = (jnp.zeros((HIDDEN_WIDTH * HIDDEN_WIDTH, EDGE_FEATURES), jnp.float32), jnp.zeros((ALIGN_ROWS, AMINO_TOTAL, HIDDEN_WIDTH), jnp.float32))
    (tensor_final_accrual, target_adjoint), source_pieces = lax.scan(backward_block, starting_tensor, (source_tiles, grad_blocks))
    source_adjoint = jnp.transpose(source_pieces, (1, 0, 2, 3)).reshape(ALIGN_ROWS, AMINO_TOTAL, HIDDEN_WIDTH)
    alignment_mapped_adjoint = truncated_numbers(jnp.concatenate([source_adjoint, target_adjoint], axis=-1))
    tensor_flank_accrual = jnp.einsum('ctm,ctg->mg', alignment_standardized.astype(jnp.float32), alignment_mapped_adjoint.astype(jnp.float32))
    alignment_standard_adjoint = jnp.dot(alignment_mapped_adjoint, tensor_flank_matrix.T, preferred_element_type=jnp.float32)
    alignment_adjoint = truncated_numbers(standardizer_adjoint(alignment_embedding.astype(jnp.float32), alignment_standard_adjoint, -1))
    return (edge_embedding_updated, edge_embedding_adjoint, alignment_adjoint, tensor_flank_accrual / AMINO_TOTAL, tensor_final_accrual / AMINO_TOTAL, outward_sigmoid_accrual / AMINO_TOTAL, outward_final_accrual / AMINO_TOTAL, inward_sigmoid_accrual / AMINO_TOTAL, inward_final_accrual / AMINO_TOTAL)
```

```python
import jax
import jax.numpy as jnp
from jax import lax
from jax.sharding import PartitionSpec as P

EPSILON = 1e-05


def truncated_numbers(values):
    return lax.optimization_barrier(values.astype(jnp.bfloat16))


def edge_standardized(values, which_axis):
    average = jnp.mean(values, axis=which_axis, keepdims=True)
    centred = values - average
    factor = lax.rsqrt(jnp.mean(centred * centred, axis=which_axis, keepdims=True) + EPSILON)
    return centred * factor


def standardizer_adjoint(values, gradient, which_axis):
    average = jnp.mean(values, axis=which_axis, keepdims=True)
    centred = values - average
    factor = lax.rsqrt(jnp.mean(centred * centred, axis=which_axis, keepdims=True) + EPSILON)
    hatted = centred * factor
    return factor * (
        gradient
        - jnp.mean(gradient, axis=which_axis, keepdims=True)
        - hatted * jnp.mean(gradient * hatted, axis=which_axis, keepdims=True)
    )


def sigmoid_pieces(edge_entry, linear_mapping, latent_tensor):
    standardized_edges = truncated_numbers(edge_standardized(edge_entry.astype(jnp.float32), 2))
    gate_pre = jnp.dot(
        standardized_edges,
        linear_mapping[:, 4 * latent_tensor :],
        preferred_element_type=jnp.float32,
    )
    split_pre = jnp.einsum(
        "rnz,zc->crn",
        standardized_edges,
        linear_mapping[:, : 4 * latent_tensor],
        preferred_element_type=jnp.float32,
    )
    source_masked = truncated_numbers(
        jax.nn.sigmoid(split_pre[:latent_tensor]) * split_pre[latent_tensor : 2 * latent_tensor]
    )
    target_masked = truncated_numbers(
        jax.nn.sigmoid(split_pre[2 * latent_tensor : 3 * latent_tensor])
        * split_pre[3 * latent_tensor :]
    )
    return (standardized_edges, gate_pre, split_pre, source_masked, target_masked)


def grouped(values, groups):
    return values.reshape((groups, values.shape[0] // groups) + values.shape[1:])


def gathered(values, axis):
    groups = lax.axis_size("dap")
    copies = jnp.broadcast_to(values[None], (groups,) + values.shape)
    return jnp.moveaxis(lax.all_to_all(copies, "dap", 0, 0, tiled=True), 0, axis)


def exchanged(values):
    return lax.all_to_all(values, "dap", split_axis=0, concat_axis=0, tiled=True)


def totalled(parts):
    groups = lax.axis_size("dap")
    flat = jnp.concatenate([part.reshape(-1) for part in parts])
    unit = groups * 16 * 128
    padded = -(-flat.size // unit) * unit
    blocks = jnp.pad(flat, (0, padded - flat.size)).reshape(groups, -1, 128)
    mine = exchanged(truncated_numbers(blocks)).astype(jnp.float32).sum(axis=0)
    whole = gathered(truncated_numbers(mine), 0).astype(jnp.float32).reshape(-1)
    out, place = [], 0
    for part in parts:
        out.append(whole[place : place + part.size].reshape(part.shape))
        place += part.size
    return out


def to_channels(*rows):
    groups = lax.axis_size("dap")
    packed = jnp.stack([grouped(values, groups) for values in rows], axis=1)
    received = exchanged(packed)
    return [
        jnp.moveaxis(received[:, at], 0, 1).reshape(
            received.shape[2], -1, received.shape[4]
        )[None]
        for at in range(len(rows))
    ]


def to_rows(*columns):
    groups = lax.axis_size("dap")
    packed = jnp.stack(
        [
            jnp.moveaxis(
                values[0].reshape(values.shape[1], groups, -1, values.shape[3]), 1, 0
            )
            for values in columns
        ],
        axis=1,
    )
    received = exchanged(packed)
    return [
        received[:, at].reshape((-1,) + received.shape[3:]) for at in range(len(columns))
    ]


def contract_items(left_cols, right_cols, outgoing):
    if outgoing:
        return jnp.einsum(
            "xqik,xqjk->xqij", left_cols, right_cols, preferred_element_type=jnp.float32
        )
    return jnp.einsum("xqki,xqkj->xqij", left_cols, right_cols, preferred_element_type=jnp.float32)


def contract_back_items(grad_cols, left_cols, right_cols, outgoing):
    if outgoing:
        source_adjoint = jnp.einsum(
            "xqij,xqjk->xqik", grad_cols, right_cols, preferred_element_type=jnp.float32
        )
        target_adjoint = jnp.einsum(
            "xqij,xqik->xqjk", grad_cols, left_cols, preferred_element_type=jnp.float32
        )
    else:
        source_adjoint = jnp.einsum(
            "xqij,xqkj->xqki", grad_cols, right_cols, preferred_element_type=jnp.float32
        )
        target_adjoint = jnp.einsum(
            "xqij,xqki->xqkj", grad_cols, left_cols, preferred_element_type=jnp.float32
        )
    return (truncated_numbers(source_adjoint), truncated_numbers(target_adjoint))


def triangle_forward(edge_entry, linear_mapping, final, outgoing):
    latent_tensor = final.shape[0]
    groups = lax.axis_size("dap")
    standardized_edges, gate_pre, split_pre, source_masked, target_masked = sigmoid_pieces(
        edge_entry, linear_mapping, latent_tensor
    )
    kept = to_channels(source_masked, target_masked)
    triangle_cols = truncated_numbers(contract_items(kept[0], kept[1], outgoing))
    (triangle,) = to_rows(triangle_cols)
    unit_norm = truncated_numbers(edge_standardized(triangle.astype(jnp.float32), 0))
    values = jnp.einsum("crn,cz->rnz", unit_norm, final, preferred_element_type=jnp.float32)
    pair_new = truncated_numbers(edge_entry.astype(jnp.float32) + jax.nn.sigmoid(gate_pre) * values)
    return (pair_new, triangle, kept)


def triangle_back(edge_entry, linear_mapping, final, outgoing, triangle, kept, gradient):
    latent_tensor = final.shape[0]
    groups = lax.axis_size("dap")
    standardized_edges, gate_pre, split_pre, source_masked, target_masked = sigmoid_pieces(
        edge_entry, linear_mapping, latent_tensor
    )
    sigmoid_factor = jax.nn.sigmoid(gate_pre)
    tri_wide = triangle.astype(jnp.float32)
    unit_norm = truncated_numbers(edge_standardized(tri_wide, 0))
    values = jnp.einsum("crn,cz->rnz", unit_norm, final, preferred_element_type=jnp.float32)
    scaled = truncated_numbers(gradient * sigmoid_factor)
    final_sum = jnp.einsum("crn,rnz->cz", unit_norm, scaled, preferred_element_type=jnp.float32)
    grad_unit = jnp.einsum("rnz,cz->crn", scaled, final, preferred_element_type=jnp.float32)
    adjoint_sigmoid = truncated_numbers(gradient * values * sigmoid_factor * (1.0 - sigmoid_factor))
    grad_triangle = truncated_numbers(standardizer_adjoint(tri_wide, grad_unit, 0))
    (gradient_cols,) = to_channels(grad_triangle)
    left_back, right_back = contract_back_items(gradient_cols, kept[0], kept[1], outgoing)
    source_adjoint, target_adjoint = [
        values.astype(jnp.float32) for values in to_rows(left_back, right_back)
    ]
    logistic_primary = jax.nn.sigmoid(split_pre[:latent_tensor])
    logistic_tertiary = jax.nn.sigmoid(split_pre[2 * latent_tensor : 3 * latent_tensor])
    grad_split = truncated_numbers(
        jnp.concatenate(
            [
                source_adjoint
                * split_pre[latent_tensor : 2 * latent_tensor]
                * logistic_primary
                * (1.0 - logistic_primary),
                source_adjoint * logistic_primary,
                target_adjoint
                * split_pre[3 * latent_tensor :]
                * logistic_tertiary
                * (1.0 - logistic_tertiary),
                target_adjoint * logistic_tertiary,
            ],
            axis=0,
        )
    )
    proj_sum = jnp.concatenate(
        [
            jnp.einsum(
                "rnz,crn->zc", standardized_edges, grad_split, preferred_element_type=jnp.float32
            ),
            jnp.einsum(
                "rnz,rnc->zc",
                standardized_edges,
                adjoint_sigmoid,
                preferred_element_type=jnp.float32,
            ),
        ],
        axis=1,
    )
    grad_norm = jnp.einsum(
        "crn,zc->rnz",
        grad_split,
        linear_mapping[:, : 4 * latent_tensor],
        preferred_element_type=jnp.float32,
    )
    grad_norm = grad_norm + jnp.dot(
        adjoint_sigmoid,
        linear_mapping[:, 4 * latent_tensor :].T,
        preferred_element_type=jnp.float32,
    )
    grad_pair = gradient + standardizer_adjoint(edge_entry.astype(jnp.float32), grad_norm, 2)
    return (grad_pair, proj_sum, final_sum)


def shards(
    edge_embedding,
    alignment_embedding,
    tensor_flank_matrix,
    tensor_final_matrix,
    outward_sigmoid_matrix,
    outward_final_matrix,
    inward_sigmoid_matrix,
    inward_final_matrix,
    adjoint_seed,
):
    rows_here = edge_embedding.shape[0]
    residues = edge_embedding.shape[1]
    alignment_depth = alignment_embedding.shape[0]
    contraction_extent = tensor_flank_matrix.shape[1] // 2
    alignment_standardized = truncated_numbers(
        edge_standardized(alignment_embedding.astype(jnp.float32), 2)
    )
    alignment_mapped = jnp.dot(
        alignment_standardized, tensor_flank_matrix, preferred_element_type=jnp.float32
    )
    tensor_source_factor = truncated_numbers(alignment_mapped[..., :contraction_extent])
    tensor_target_factor = truncated_numbers(alignment_mapped[..., contraction_extent:])
    right_all = gathered(tensor_target_factor, 1).reshape(
        alignment_depth, residues, contraction_extent
    )
    tile_lines = 128 if residues % 128 == 0 else residues
    tile_number = residues // tile_lines
    outer_parts = []
    first_parts = []
    for block_index in range(tile_number):
        lower = block_index * tile_lines
        right_block = right_all[:, lower : lower + tile_lines]
        triangle_contraction = jnp.einsum(
            "sic,sjd->ijcd", tensor_source_factor, right_block, preferred_element_type=jnp.float32
        )
        outer_block = truncated_numbers(
            triangle_contraction.reshape(
                rows_here, tile_lines, contraction_extent * contraction_extent
            )
            / alignment_depth
        )
        update = jnp.dot(outer_block, tensor_final_matrix, preferred_element_type=jnp.float32)
        first_parts.append(
            truncated_numbers(
                edge_embedding[:, lower : lower + tile_lines].astype(jnp.float32) + update
            )
        )
        outer_parts.append(outer_block)
    outer_mean = jnp.concatenate(outer_parts, axis=1)
    pair_one = jnp.concatenate(first_parts, axis=1)
    pair_two, triangle_out, kept_out = triangle_forward(
        pair_one, outward_sigmoid_matrix, outward_final_matrix, True
    )
    edge_embedding_updated, triangle_in, kept_in = triangle_forward(
        pair_two, inward_sigmoid_matrix, inward_final_matrix, False
    )
    grad_two, inward_sigmoid_accrual, inward_final_accrual = triangle_back(
        pair_two,
        inward_sigmoid_matrix,
        inward_final_matrix,
        False,
        triangle_in,
        kept_in,
        adjoint_seed.astype(jnp.float32),
    )
    grad_one, outward_sigmoid_accrual, outward_final_accrual = triangle_back(
        pair_one, outward_sigmoid_matrix, outward_final_matrix, True, triangle_out, kept_out, grad_two
    )
    edge_embedding_adjoint = truncated_numbers(grad_one)
    tensor_final_accrual = jnp.einsum(
        "rnk,rnz->kz", outer_mean, edge_embedding_adjoint, preferred_element_type=jnp.float32
    )
    source_adjoint = jnp.zeros((alignment_depth, rows_here, contraction_extent), jnp.float32)
    outer_grads = []
    for block_index in range(tile_number):
        lower = block_index * tile_lines
        right_block = right_all[:, lower : lower + tile_lines]
        adjoint_tensor_mean = truncated_numbers(
            jnp.dot(
                edge_embedding_adjoint[:, lower : lower + tile_lines],
                tensor_final_matrix.T,
                preferred_element_type=jnp.float32,
            )
        )
        adjoint_tensor_mean = adjoint_tensor_mean.reshape(
            rows_here, tile_lines, contraction_extent, contraction_extent
        )
        source_adjoint = (
            source_adjoint
            + jnp.einsum(
                "mopz,loz->lmp",
                adjoint_tensor_mean,
                right_block,
                preferred_element_type=jnp.float32,
            )
            / alignment_depth
        )
        outer_grads.append(adjoint_tensor_mean)
    pair_columns = lax.all_to_all(
        edge_embedding_adjoint, "dap", split_axis=1, concat_axis=0, tiled=True
    )
    left_all = gathered(tensor_source_factor, 1).reshape(
        alignment_depth, residues, contraction_extent
    )
    target_adjoint = jnp.zeros((alignment_depth, rows_here, contraction_extent), jnp.float32)
    for block_index in range(tile_number):
        lower = block_index * tile_lines
        column_grad = truncated_numbers(
            jnp.dot(
                pair_columns[lower : lower + tile_lines],
                tensor_final_matrix.T,
                preferred_element_type=jnp.float32,
            )
        )
        column_grad = column_grad.reshape(
            tile_lines, rows_here, contraction_extent, contraction_extent
        )
        target_adjoint = (
            target_adjoint
            + jnp.einsum(
                "gxqp,vgq->vxp",
                column_grad,
                left_all[:, lower : lower + tile_lines],
                preferred_element_type=jnp.float32,
            )
            / alignment_depth
        )
    alignment_mapped_adjoint = truncated_numbers(
        jnp.concatenate([source_adjoint, target_adjoint], axis=2)
    )
    tensor_flank_accrual = jnp.einsum(
        "ajo,ajm->om",
        alignment_standardized,
        alignment_mapped_adjoint,
        preferred_element_type=jnp.float32,
    )
    alignment_standard_adjoint = jnp.dot(
        alignment_mapped_adjoint, tensor_flank_matrix.T, preferred_element_type=jnp.float32
    )
    alignment_adjoint = truncated_numbers(
        standardizer_adjoint(alignment_embedding.astype(jnp.float32), alignment_standard_adjoint, 2)
    )
    totals = totalled(
        (
            tensor_flank_accrual,
            tensor_final_accrual,
            outward_sigmoid_accrual,
            outward_final_accrual,
            inward_sigmoid_accrual,
            inward_final_accrual,
        )
    )
    return (
        edge_embedding_updated,
        edge_embedding_adjoint,
        alignment_adjoint,
        totals[0] / residues,
        totals[1] / residues,
        totals[2] / residues,
        totals[3] / residues,
        totals[4] / residues,
        totals[5] / residues,
    )


def solution(mesh):
    placed = (
        P(("dp", "dap"), None, None),
        P("dp", "dap", None),
        P(),
        P(),
        P(),
        P(),
        P(),
        P(),
        P(("dp", "dap"), None, None),
    )
    return jax.shard_map(
        shards,
        mesh=mesh,
        in_specs=placed,
        out_specs=(
            P(("dp", "dap"), None, None),
            P(("dp", "dap"), None, None),
            P("dp", "dap", None),
            P("dp", None),
            P("dp", None),
            P("dp", None),
            P("dp", None),
            P("dp", None),
            P("dp", None),
        ),
        check_vma=False,
    )
```

```python
from functools import partial

import jax
import jax.numpy as jnp
from jax import lax
from jax.experimental import pallas as pl
from jax.experimental.pallas import tpu as pltpu
from jax.sharding import PartitionSpec as P

EPSILON = 1e-05


def truncated_numbers(values):
    return lax.optimization_barrier(values.astype(jnp.bfloat16))


def edge_standardized(values, which_axis):
    average = jnp.mean(values, axis=which_axis, keepdims=True)
    centred = values - average
    factor = lax.rsqrt(jnp.mean(centred * centred, axis=which_axis, keepdims=True) + EPSILON)
    return centred * factor


def standardizer_adjoint(values, gradient, which_axis):
    average = jnp.mean(values, axis=which_axis, keepdims=True)
    centred = values - average
    factor = lax.rsqrt(jnp.mean(centred * centred, axis=which_axis, keepdims=True) + EPSILON)
    hatted = centred * factor
    return factor * (
        gradient
        - jnp.mean(gradient, axis=which_axis, keepdims=True)
        - hatted * jnp.mean(gradient * hatted, axis=which_axis, keepdims=True)
    )


def sigmoid_pieces(edge_entry, linear_mapping, latent_tensor):
    standardized_edges = truncated_numbers(edge_standardized(edge_entry.astype(jnp.float32), 2))
    gate_pre = jnp.dot(
        standardized_edges,
        linear_mapping[:, 4 * latent_tensor :],
        preferred_element_type=jnp.float32,
    )
    split_pre = jnp.einsum(
        "rnz,zc->crn",
        standardized_edges,
        linear_mapping[:, : 4 * latent_tensor],
        preferred_element_type=jnp.float32,
    )
    source_masked = truncated_numbers(
        jax.nn.sigmoid(split_pre[:latent_tensor]) * split_pre[latent_tensor : 2 * latent_tensor]
    )
    target_masked = truncated_numbers(
        jax.nn.sigmoid(split_pre[2 * latent_tensor : 3 * latent_tensor])
        * split_pre[3 * latent_tensor :]
    )
    return (standardized_edges, gate_pre, split_pre, source_masked, target_masked)


def grouped(values, groups):
    return values.reshape((groups, values.shape[0] // groups) + values.shape[1:])


def gathered(values, axis):
    groups = lax.axis_size("dap")
    copies = jnp.broadcast_to(values[None], (groups,) + values.shape)
    return jnp.moveaxis(lax.all_to_all(copies, "dap", 0, 0, tiled=True), 0, axis)


def exchanged(values):
    return lax.all_to_all(values, "dap", split_axis=0, concat_axis=0, tiled=True)


def totalled(parts):
    groups = lax.axis_size("dap")
    flat = jnp.concatenate([part.reshape(-1) for part in parts])
    unit = groups * 16 * 128
    padded = -(-flat.size // unit) * unit
    blocks = jnp.pad(flat, (0, padded - flat.size)).reshape(groups, -1, 128)
    mine = exchanged(truncated_numbers(blocks)).astype(jnp.float32).sum(axis=0)
    whole = gathered(truncated_numbers(mine), 0).astype(jnp.float32).reshape(-1)
    out, place = [], 0
    for part in parts:
        out.append(whole[place : place + part.size].reshape(part.shape))
        place += part.size
    return out


def to_channels(*rows):
    groups = lax.axis_size("dap")
    packed = jnp.stack([grouped(values, groups) for values in rows], axis=1)
    received = exchanged(packed)
    return [
        jnp.moveaxis(received[:, at], 0, 1).reshape(
            received.shape[2], -1, received.shape[4]
        )[None]
        for at in range(len(rows))
    ]


def to_rows(*columns):
    groups = lax.axis_size("dap")
    packed = jnp.stack(
        [
            jnp.moveaxis(
                values[0].reshape(values.shape[1], groups, -1, values.shape[3]), 1, 0
            )
            for values in columns
        ],
        axis=1,
    )
    received = exchanged(packed)
    return [
        received[:, at].reshape((-1,) + received.shape[3:]) for at in range(len(columns))
    ]


def contract_items(left_cols, right_cols, outgoing):
    if outgoing:
        return jnp.einsum(
            "xqik,xqjk->xqij", left_cols, right_cols, preferred_element_type=jnp.float32
        )
    return jnp.einsum("xqki,xqkj->xqij", left_cols, right_cols, preferred_element_type=jnp.float32)


def contract_back_items(grad_cols, left_cols, right_cols, outgoing):
    if outgoing:
        source_adjoint = jnp.einsum(
            "xqij,xqjk->xqik", grad_cols, right_cols, preferred_element_type=jnp.float32
        )
        target_adjoint = jnp.einsum(
            "xqij,xqik->xqjk", grad_cols, left_cols, preferred_element_type=jnp.float32
        )
    else:
        source_adjoint = jnp.einsum(
            "xqij,xqkj->xqki", grad_cols, right_cols, preferred_element_type=jnp.float32
        )
        target_adjoint = jnp.einsum(
            "xqij,xqki->xqkj", grad_cols, left_cols, preferred_element_type=jnp.float32
        )
    return (truncated_numbers(source_adjoint), truncated_numbers(target_adjoint))


def triangle_forward(edge_entry, linear_mapping, final, outgoing):
    latent_tensor = final.shape[0]
    groups = lax.axis_size("dap")
    standardized_edges, gate_pre, split_pre, source_masked, target_masked = sigmoid_pieces(
        edge_entry, linear_mapping, latent_tensor
    )
    kept = to_channels(source_masked, target_masked)
    triangle_cols = truncated_numbers(contract_items(kept[0], kept[1], outgoing))
    (triangle,) = to_rows(triangle_cols)
    unit_norm = truncated_numbers(edge_standardized(triangle.astype(jnp.float32), 0))
    values = jnp.einsum("crn,cz->rnz", unit_norm, final, preferred_element_type=jnp.float32)
    pair_new = truncated_numbers(edge_entry.astype(jnp.float32) + jax.nn.sigmoid(gate_pre) * values)
    return (pair_new, triangle, kept)


def triangle_back(edge_entry, linear_mapping, final, outgoing, triangle, kept, gradient):
    latent_tensor = final.shape[0]
    groups = lax.axis_size("dap")
    standardized_edges, gate_pre, split_pre, source_masked, target_masked = sigmoid_pieces(
        edge_entry, linear_mapping, latent_tensor
    )
    sigmoid_factor = jax.nn.sigmoid(gate_pre)
    tri_wide = triangle.astype(jnp.float32)
    unit_norm = truncated_numbers(edge_standardized(tri_wide, 0))
    values = jnp.einsum("crn,cz->rnz", unit_norm, final, preferred_element_type=jnp.float32)
    scaled = truncated_numbers(gradient * sigmoid_factor)
    final_sum = jnp.einsum("crn,rnz->cz", unit_norm, scaled, preferred_element_type=jnp.float32)
    grad_unit = jnp.einsum("rnz,cz->crn", scaled, final, preferred_element_type=jnp.float32)
    adjoint_sigmoid = truncated_numbers(gradient * values * sigmoid_factor * (1.0 - sigmoid_factor))
    grad_triangle = truncated_numbers(standardizer_adjoint(tri_wide, grad_unit, 0))
    (gradient_cols,) = to_channels(grad_triangle)
    left_back, right_back = contract_back_items(gradient_cols, kept[0], kept[1], outgoing)
    source_adjoint, target_adjoint = [
        values.astype(jnp.float32) for values in to_rows(left_back, right_back)
    ]
    logistic_primary = jax.nn.sigmoid(split_pre[:latent_tensor])
    logistic_tertiary = jax.nn.sigmoid(split_pre[2 * latent_tensor : 3 * latent_tensor])
    grad_split = truncated_numbers(
        jnp.concatenate(
            [
                source_adjoint
                * split_pre[latent_tensor : 2 * latent_tensor]
                * logistic_primary
                * (1.0 - logistic_primary),
                source_adjoint * logistic_primary,
                target_adjoint
                * split_pre[3 * latent_tensor :]
                * logistic_tertiary
                * (1.0 - logistic_tertiary),
                target_adjoint * logistic_tertiary,
            ],
            axis=0,
        )
    )
    proj_sum = jnp.concatenate(
        [
            jnp.einsum(
                "rnz,crn->zc", standardized_edges, grad_split, preferred_element_type=jnp.float32
            ),
            jnp.einsum(
                "rnz,rnc->zc",
                standardized_edges,
                adjoint_sigmoid,
                preferred_element_type=jnp.float32,
            ),
        ],
        axis=1,
    )
    grad_norm = jnp.einsum(
        "crn,zc->rnz",
        grad_split,
        linear_mapping[:, : 4 * latent_tensor],
        preferred_element_type=jnp.float32,
    )
    grad_norm = grad_norm + jnp.dot(
        adjoint_sigmoid,
        linear_mapping[:, 4 * latent_tensor :].T,
        preferred_element_type=jnp.float32,
    )
    grad_pair = gradient + standardizer_adjoint(edge_entry.astype(jnp.float32), grad_norm, 2)
    return (grad_pair, proj_sum, final_sum)


def shards(
    edge_embedding,
    alignment_embedding,
    tensor_flank_matrix,
    tensor_final_matrix,
    outward_sigmoid_matrix,
    outward_final_matrix,
    inward_sigmoid_matrix,
    inward_final_matrix,
    adjoint_seed,
):
    rows_here = edge_embedding.shape[0]
    residues = edge_embedding.shape[1]
    alignment_depth = alignment_embedding.shape[0]
    contraction_extent = tensor_flank_matrix.shape[1] // 2
    alignment_standardized = truncated_numbers(
        edge_standardized(alignment_embedding.astype(jnp.float32), 2)
    )
    alignment_mapped = jnp.dot(
        alignment_standardized, tensor_flank_matrix, preferred_element_type=jnp.float32
    )
    tensor_source_factor = truncated_numbers(alignment_mapped[..., :contraction_extent])
    tensor_target_factor = truncated_numbers(alignment_mapped[..., contraction_extent:])
    right_all = gathered(tensor_target_factor, 1).reshape(
        alignment_depth, residues, contraction_extent
    )
    tile_lines = 128 if residues % 128 == 0 else residues
    tile_number = residues // tile_lines
    outer_parts = []
    first_parts = []
    for block_index in range(tile_number):
        lower = block_index * tile_lines
        right_block = right_all[:, lower : lower + tile_lines]
        triangle_contraction = jnp.einsum(
            "sic,sjd->ijcd", tensor_source_factor, right_block, preferred_element_type=jnp.float32
        )
        outer_block = truncated_numbers(
            triangle_contraction.reshape(
                rows_here, tile_lines, contraction_extent * contraction_extent
            )
            / alignment_depth
        )
        update = jnp.dot(outer_block, tensor_final_matrix, preferred_element_type=jnp.float32)
        first_parts.append(
            truncated_numbers(
                edge_embedding[:, lower : lower + tile_lines].astype(jnp.float32) + update
            )
        )
        outer_parts.append(outer_block)
    outer_mean = jnp.concatenate(outer_parts, axis=1)
    pair_one = jnp.concatenate(first_parts, axis=1)
    pair_two, triangle_out, kept_out = triangle_forward(
        pair_one, outward_sigmoid_matrix, outward_final_matrix, True
    )
    edge_embedding_updated, triangle_in, kept_in = triangle_forward(
        pair_two, inward_sigmoid_matrix, inward_final_matrix, False
    )
    grad_two, inward_sigmoid_accrual, inward_final_accrual = triangle_back(
        pair_two,
        inward_sigmoid_matrix,
        inward_final_matrix,
        False,
        triangle_in,
        kept_in,
        adjoint_seed.astype(jnp.float32),
    )
    grad_one, outward_sigmoid_accrual, outward_final_accrual = triangle_back(
        pair_one, outward_sigmoid_matrix, outward_final_matrix, True, triangle_out, kept_out, grad_two
    )
    edge_embedding_adjoint = truncated_numbers(grad_one)
    tensor_final_accrual = jnp.einsum(
        "rnk,rnz->kz", outer_mean, edge_embedding_adjoint, preferred_element_type=jnp.float32
    )
    source_adjoint = jnp.zeros((alignment_depth, rows_here, contraction_extent), jnp.float32)
    outer_grads = []
    for block_index in range(tile_number):
        lower = block_index * tile_lines
        right_block = right_all[:, lower : lower + tile_lines]
        adjoint_tensor_mean = truncated_numbers(
            jnp.dot(
                edge_embedding_adjoint[:, lower : lower + tile_lines],
                tensor_final_matrix.T,
                preferred_element_type=jnp.float32,
            )
        )
        adjoint_tensor_mean = adjoint_tensor_mean.reshape(
            rows_here, tile_lines, contraction_extent, contraction_extent
        )
        source_adjoint = (
            source_adjoint
            + jnp.einsum(
                "mopz,loz->lmp",
                adjoint_tensor_mean,
                right_block,
                preferred_element_type=jnp.float32,
            )
            / alignment_depth
        )
        outer_grads.append(adjoint_tensor_mean)
    pair_columns = lax.all_to_all(
        edge_embedding_adjoint, "dap", split_axis=1, concat_axis=0, tiled=True
    )
    left_all = gathered(tensor_source_factor, 1).reshape(
        alignment_depth, residues, contraction_extent
    )
    target_adjoint = jnp.zeros((alignment_depth, rows_here, contraction_extent), jnp.float32)
    for block_index in range(tile_number):
        lower = block_index * tile_lines
        column_grad = truncated_numbers(
            jnp.dot(
                pair_columns[lower : lower + tile_lines],
                tensor_final_matrix.T,
                preferred_element_type=jnp.float32,
            )
        )
        column_grad = column_grad.reshape(
            tile_lines, rows_here, contraction_extent, contraction_extent
        )
        target_adjoint = (
            target_adjoint
            + jnp.einsum(
                "gxqp,vgq->vxp",
                column_grad,
                left_all[:, lower : lower + tile_lines],
                preferred_element_type=jnp.float32,
            )
            / alignment_depth
        )
    alignment_mapped_adjoint = truncated_numbers(
        jnp.concatenate([source_adjoint, target_adjoint], axis=2)
    )
    tensor_flank_accrual = jnp.einsum(
        "ajo,ajm->om",
        alignment_standardized,
        alignment_mapped_adjoint,
        preferred_element_type=jnp.float32,
    )
    alignment_standard_adjoint = jnp.dot(
        alignment_mapped_adjoint, tensor_flank_matrix.T, preferred_element_type=jnp.float32
    )
    alignment_adjoint = truncated_numbers(
        standardizer_adjoint(alignment_embedding.astype(jnp.float32), alignment_standard_adjoint, 2)
    )
    totals = totalled(
        (
            tensor_flank_accrual,
            tensor_final_accrual,
            outward_sigmoid_accrual,
            outward_final_accrual,
            inward_sigmoid_accrual,
            inward_final_accrual,
        )
    )
    return (
        edge_embedding_updated,
        edge_embedding_adjoint,
        alignment_adjoint,
        totals[0] / residues,
        totals[1] / residues,
        totals[2] / residues,
        totals[3] / residues,
        totals[4] / residues,
        totals[5] / residues,
    )


F32 = jnp.float32
BF16 = jnp.bfloat16
LANES = 128
SUB = 8


def nn(a, b):
    return lax.dot_general(a, b, (((1,), (0,)), ((), ())), preferred_element_type=F32)


def nt(a, b):
    return lax.dot_general(a, b, (((1,), (1,)), ((), ())), preferred_element_type=F32)


def tn(a, b):
    return lax.dot_general(a, b, (((0,), (0,)), ((), ())), preferred_element_type=F32)


def launch(body, outs, args, scratch=(), name=None, flops=2e8):
    vmem = pl.BlockSpec(memory_space=pltpu.VMEM)
    moved = sum(a.size * a.dtype.itemsize for a in args) + sum(
        o.size * o.dtype.itemsize for o in outs
    )
    return pl.pallas_call(
        body,
        out_shape=outs,
        in_specs=[vmem] * len(args),
        out_specs=[vmem] * len(outs),
        scratch_shapes=list(scratch),
        name=name,
        cost_estimate=pl.CostEstimate(
            flops=int(flops), bytes_accessed=int(moved), transcendentals=0
        ),
        compiler_params=pltpu.CompilerParams(vmem_limit_bytes=40 * 1024 * 1024),
    )(*args)


def moments(x, axis):
    average = jnp.mean(x, axis=axis, keepdims=True)
    centred = x - average
    factor = lax.rsqrt(jnp.mean(centred * centred, axis=axis, keepdims=True) + EPSILON)
    return centred * factor, factor


def moments_adjoint(hatted, factor, gradient, axis):
    return factor * (
        gradient
        - jnp.mean(gradient, axis=axis, keepdims=True)
        - hatted * jnp.mean(gradient * hatted, axis=axis, keepdims=True)
    )


def tall(x):
    return jnp.concatenate([x, jnp.zeros((LANES - x.shape[0], x.shape[1]), x.dtype)], axis=0)


def dealt(x, groups):
    return x.reshape((groups, x.shape[0] // groups) + x.shape[1:])


def gated_pair(projected, width):
    left = jax.nn.sigmoid(projected[:width]) * projected[width : 2 * width]
    right = jax.nn.sigmoid(projected[2 * width : 3 * width]) * projected[3 * width : 4 * width]
    return left, right


def send_pair(out_ref, row, left, right, groups):
    both = jnp.concatenate([dealt(left, groups), dealt(right, groups)], axis=1)
    wide = both.shape[1]
    out_ref[:, row * wide : (row + 1) * wide, :] = both.astype(BF16)


def msa_kernel(sizes, msa_ref, flank_t_ref, send_ref, normal_ref, left_ref):
    rows, depth, hidden, groups = sizes
    for row in range(rows):
        hatted, _ = moments(msa_ref[row].astype(F32), 1)
        normal = hatted.astype(BF16)
        normal_ref[row] = normal
        twice = jnp.concatenate([normal, normal], axis=0)
        mapped = nt(flank_t_ref[...], twice)
        lane = lax.broadcasted_iota(jnp.int32, (hidden, LANES), 1)
        low = lane < depth
        left = mapped[:hidden]
        left_ref[row * hidden : (row + 1) * hidden] = jnp.where(low, left, 0.0).astype(BF16)
        left_ref[(rows + row) * hidden : (rows + row + 1) * hidden] = jnp.where(
            low, 0.0, left
        ).astype(BF16)
        half = hidden // 2
        right = jnp.where(
            low[:half], mapped[hidden : hidden + half], mapped[hidden + half :]
        ).astype(BF16)
        for group in range(groups):
            send_ref[group, row * half : (row + 1) * half, :] = right


def outer_kernel(
    sizes,
    right_ref,
    left_ref,
    edge_ref,
    final_t_ref,
    gates_t_ref,
    send_ref,
    spread_ref,
    outer_ref,
    pair_ref,
    wide_ref,
):
    rows, residues, depth, hidden, groups, width = sizes
    half = hidden // 2
    wide_ref[...] = right_ref[...].reshape(wide_ref.shape).astype(F32)
    for d in range(half):
        picked = wide_ref[pl.ds(d, residues, stride=half), :]
        spread_ref[d * LANES : (d + 1) * LANES, :] = tall(picked).astype(BF16)
    for d in range(0, half, 2):
        block = nt(left_ref[...], spread_ref[d * LANES : (d + 2) * LANES, :]) / depth
        for e in range(2):
            for h in range(2):
                for row in range(rows):
                    at = (h * rows + row) * hidden
                    to = (h * half + d + e) * hidden
                    outer_ref[to : to + hidden, row * LANES : (row + 1) * LANES] = block[
                        at : at + hidden, e * LANES : (e + 1) * LANES
                    ].astype(BF16)
    update = nn(final_t_ref[...], outer_ref[...])
    for row in range(rows):
        lanes = slice(row * LANES, (row + 1) * LANES)
        entry = tall(edge_ref[row].astype(F32)).T
        pair = (entry + update[:, lanes]).astype(BF16)
        pair_ref[:, lanes] = pair
        hatted, _ = moments(pair.astype(F32), 0)
        projected = nn(gates_t_ref[: 4 * width, :], hatted.astype(BF16))
        left, right = gated_pair(projected, width)
        send_pair(send_ref, row, left, right, groups)


def triangle_kernel(sizes, outgoing, both_ref, send_ref, wide_ref, result_ref):
    residues, share = sizes
    wide_ref[...] = both_ref[...].reshape(wide_ref.shape).astype(F32)
    for c in range(share):
        left = wide_ref[pl.ds(c, residues, stride=2 * share), :].astype(BF16)
        right = wide_ref[pl.ds(share + c, residues, stride=2 * share), :].astype(BF16)
        if outgoing:
            product = nt(left, tall(right))
        else:
            product = tn(left, right)[:residues]
        result_ref[pl.ds(c, residues, stride=share), :] = product
    send_ref[...] = result_ref[...].astype(BF16).reshape(send_ref.shape)


def triangle_adjoint_kernel(
    sizes, outgoing, both_ref, grad_ref, send_ref, wide_ref, tri_ref, result_ref
):
    residues, share, rows, riders = sizes
    own = rows * share
    wide_ref[...] = both_ref[...].reshape(wide_ref.shape).astype(F32)
    tri_ref[...] = grad_ref[:, :own, :].astype(F32).reshape(tri_ref.shape)
    for c in range(share):
        left = wide_ref[pl.ds(c, residues, stride=2 * share), :].astype(BF16)
        right = wide_ref[pl.ds(share + c, residues, stride=2 * share), :].astype(BF16)
        grad = tri_ref[pl.ds(c, residues, stride=share), :].astype(BF16)
        if outgoing:
            grad_left = nn(grad, tall(right))
            grad_right = tn(grad, left)[:residues]
        else:
            grad_left = nt(right, tall(grad))
            grad_right = nn(left, tall(grad))
        result_ref[pl.ds(c, residues, stride=2 * share), :] = grad_left
        result_ref[pl.ds(share + c, residues, stride=2 * share), :] = grad_right
    groups = send_ref.shape[0]
    send_ref[:, : 2 * own, :] = (
        result_ref[...].astype(BF16).reshape(groups, 2 * own, LANES)
    )
    if riders:
        summed = jnp.sum(grad_ref[:, own:, :].astype(F32), axis=0).astype(BF16)
        for group in range(groups):
            send_ref[group, 2 * own :, :] = summed


def middle_kernel(
    sizes,
    tri_ref,
    pair_ref,
    gates_t_ref,
    final_t_ref,
    next_gates_t_ref,
    send_ref,
    next_ref,
):
    rows, groups, width = sizes
    share = width // groups
    received = tri_ref[...].astype(F32)
    for row in range(rows):
        lanes = slice(row * LANES, (row + 1) * LANES)
        tri = received[:, row * share : (row + 1) * share, :].reshape(width, LANES)
        unit, _ = moments(tri, 0)
        values = nn(final_t_ref[...], unit.astype(BF16))
        pair = pair_ref[:, lanes].astype(F32)
        hatted, _ = moments(pair, 0)
        gate = jax.nn.sigmoid(nn(gates_t_ref[4 * width :, :], hatted.astype(BF16)))
        following = (pair + gate * values).astype(BF16)
        next_ref[:, lanes] = following
        hatted, _ = moments(following.astype(F32), 0)
        projected = nn(next_gates_t_ref[: 4 * width, :], hatted.astype(BF16))
        left, right = gated_pair(projected, width)
        send_pair(send_ref, row, left, right, groups)


def tri_adjoint_row(tri, pair, gradient, gates_t_ref, final_ref, final_t_ref, width):
    hatted_tri, factor = moments(tri, 0)
    unit = hatted_tri.astype(BF16)
    values = nn(final_t_ref[...], unit)
    hatted, _ = moments(pair, 0)
    gate = jax.nn.sigmoid(nn(gates_t_ref[4 * width :, :], hatted.astype(BF16)))
    scaled = (gradient * gate).astype(BF16)
    grad_unit = nn(final_ref[...], scaled)
    grad_tri = moments_adjoint(hatted_tri, factor, grad_unit, 0)
    grad_gate = (gradient * values * gate * (1.0 - gate)).astype(BF16)
    return unit, scaled, values, gate, grad_tri, grad_gate


def turn_kernel(
    sizes,
    tri_ref,
    pair_ref,
    seed_ref,
    gates_t_ref,
    final_ref,
    final_t_ref,
    send_ref,
    out_ref,
    seed_t_ref,
    grad_gate_ref,
    final_sum_ref,
    grads_ref,
    unit_ref,
    scaled_ref,
):
    rows, residues, groups, width = sizes
    share = width // groups
    received = tri_ref[...].astype(F32)
    for row in range(rows):
        lanes = slice(row * LANES, (row + 1) * LANES)
        tri = received[:, row * share : (row + 1) * share, :].reshape(width, LANES)
        pair = pair_ref[:, lanes].astype(F32)
        gradient = tall(seed_ref[row].astype(F32)).T
        seed_t_ref[:, lanes] = gradient.astype(BF16)
        unit, scaled, values, gate, grad_tri, grad_gate = tri_adjoint_row(
            tri, pair, gradient, gates_t_ref, final_ref, final_t_ref, width
        )
        unit_ref[:, lanes] = unit
        scaled_ref[:, lanes] = scaled
        grad_gate_ref[:, lanes] = grad_gate
        grads_ref[:, row * share : (row + 1) * share, :] = dealt(grad_tri, groups)
        out_ref[row] = (pair + gate * values).T[:residues].astype(BF16)
    send_ref[...] = grads_ref[...].astype(BF16)
    final_sum_ref[...] = nt(unit_ref[...], scaled_ref[...])


def proj_adjoint_row(row, received, pair, grad_gate, gates_t_ref, gates_ref, normal_ref, proj_ref, width):
    share2 = received.shape[1]
    lanes = slice(row * LANES, (row + 1) * LANES)
    grad_left = received[:, : share2 // 2, :].reshape(width, LANES)
    grad_right = received[:, share2 // 2 :, :].reshape(width, LANES)
    hatted, factor = moments(pair, 0)
    normal = hatted.astype(BF16)
    normal_ref[:, lanes] = normal
    projected = nn(gates_t_ref[: 4 * width, :], normal)
    first = jax.nn.sigmoid(projected[:width])
    third = jax.nn.sigmoid(projected[2 * width : 3 * width])
    left_part = grad_left * first
    right_part = grad_right * third
    proj_ref[:width, lanes] = (
        left_part * projected[width : 2 * width] * (1.0 - first)
    ).astype(BF16)
    proj_ref[width : 2 * width, lanes] = left_part.astype(BF16)
    proj_ref[2 * width : 3 * width, lanes] = (
        right_part * projected[3 * width :] * (1.0 - third)
    ).astype(BF16)
    proj_ref[3 * width : 4 * width, lanes] = right_part.astype(BF16)
    proj_ref[4 * width :, lanes] = grad_gate
    grad_normal = nn(gates_ref[...], proj_ref[:, lanes])
    return moments_adjoint(hatted, factor, grad_normal, 0)


def deal_rows(out_ref, start, total, groups):
    for tile in range(total.shape[1] // LANES):
        block = dealt(total[:, tile * LANES : (tile + 1) * LANES], groups)
        out_ref[:, start : start + block.shape[1], :] = block
        start += block.shape[1]
    return start


def between_kernel(
    sizes,
    both_ref,
    pair_in_ref,
    seed_ref,
    grad_gate_in_ref,
    gates_in_t_ref,
    gates_in_ref,
    final_in_sum_ref,
    tri_ref,
    pair_out_ref,
    gates_out_t_ref,
    final_out_ref,
    final_out_t_ref,
    send_ref,
    grad_ref,
    grad_gate_ref,
    grads_ref,
    normal_ref,
    proj_ref,
    unit_ref,
    scaled_ref,
):
    rows, groups, width = sizes
    share = width // groups
    received = tri_ref[...].astype(F32)
    for row in range(rows):
        lanes = slice(row * LANES, (row + 1) * LANES)
        pair = pair_in_ref[:, lanes].astype(F32)
        both = both_ref[:, row * 2 * share : (row + 1) * 2 * share, :].astype(F32)
        gradient = seed_ref[:, lanes].astype(F32) + proj_adjoint_row(
            row,
            both,
            pair,
            grad_gate_in_ref[:, lanes],
            gates_in_t_ref,
            gates_in_ref,
            normal_ref,
            proj_ref,
            width,
        )
        grad_ref[:, lanes] = gradient
        tri = received[:, row * share : (row + 1) * share, :].reshape(width, LANES)
        unit, scaled, _, _, grad_tri, grad_gate = tri_adjoint_row(
            tri,
            pair_out_ref[:, lanes].astype(F32),
            gradient,
            gates_out_t_ref,
            final_out_ref,
            final_out_t_ref,
            width,
        )
        unit_ref[:, lanes] = unit
        scaled_ref[:, lanes] = scaled
        grad_gate_ref[:, lanes] = grad_gate
        grads_ref[:, row * share : (row + 1) * share, :] = dealt(grad_tri, groups)
    place = rows * share
    place = deal_rows(grads_ref, place, nt(normal_ref[...], proj_ref[...]), groups)
    place = deal_rows(grads_ref, place, final_in_sum_ref[...], groups)
    deal_rows(grads_ref, place, nt(unit_ref[...], scaled_ref[...]), groups)
    send_ref[...] = grads_ref[...].astype(BF16)


def gathered_rows(rest, start, tiles, width):
    out = []
    share = width // rest.shape[0]
    for tile in range(tiles):
        out.append(rest[:, start + tile * share : start + (tile + 1) * share, :].reshape(width, LANES))
    return out, start + tiles * share


def close_kernel(
    sizes,
    both_ref,
    pair_ref,
    grad_ref,
    grad_gate_ref,
    gates_t_ref,
    gates_ref,
    outer_ref,
    final_ref,
    spread_ref,
    left_ref,
    msa_normal_ref,
    send_ref,
    adjoint_ref,
    left_grad_ref,
    proj_in_ref,
    final_in_ref,
    final_out_ref,
    grads_ref,
    normal_ref,
    proj_ref,
    adjoint_t_ref,
    outer_grad_ref,
    right_grad_ref,
):
    rows, residues, depth, hidden, groups, width = sizes
    share = width // groups
    half = hidden // 2
    for row in range(rows):
        lanes = slice(row * LANES, (row + 1) * LANES)
        both = both_ref[:, row * 2 * share : (row + 1) * 2 * share, :].astype(F32)
        gradient = grad_ref[:, lanes] + proj_adjoint_row(
            row,
            both,
            pair_ref[:, lanes].astype(F32),
            grad_gate_ref[:, lanes],
            gates_t_ref,
            gates_ref,
            normal_ref,
            proj_ref,
            width,
        )
        adjoint = gradient.astype(BF16)
        adjoint_t_ref[:, lanes] = adjoint
        adjoint_ref[row] = adjoint.astype(F32).T[:residues].astype(BF16)
        spread_grad = nn(final_ref[...], adjoint).astype(BF16)
        for h in range(2):
            for d in range(half):
                at = (h * half + d) * hidden
                to = (h * rows + row) * hidden
                outer_grad_ref[to : to + hidden, d * LANES : (d + 1) * LANES] = spread_grad[
                    at : at + hidden
                ]
    for d in range(half):
        piece = tn(outer_grad_ref[:, d * LANES : (d + 1) * LANES], left_ref[...]) / depth
        right_grad_ref[pl.ds(d, residues, stride=half), :] = piece[:residues]
    own = rows * half
    grads_ref[:, :own, :] = right_grad_ref[...].reshape(groups, own, LANES)
    place = deal_rows(grads_ref, own, nt(normal_ref[...], proj_ref[...]), groups)
    outer_sum = nt(outer_ref[...], adjoint_t_ref[...])
    place = deal_rows(grads_ref, place, outer_sum, groups)
    stacked = nn(outer_grad_ref[...], spread_ref[...]) / depth
    count = rows * hidden
    lane = lax.broadcasted_iota(jnp.int32, (count, LANES), 1)
    left_grad = jnp.where(
        lane < depth, stacked[:count] + pltpu.roll(stacked[count:], LANES - depth, 1), 0.0
    ).astype(BF16)
    left_grad_ref[...] = left_grad
    flank = jnp.zeros((hidden, msa_normal_ref.shape[2]), F32)
    for row in range(rows):
        flank = flank + nn(
            left_grad[row * hidden : (row + 1) * hidden, :depth], msa_normal_ref[row]
        )
    for tile in range(flank.shape[1] // LANES):
        part = flank[:, tile * LANES : (tile + 1) * LANES].reshape(hidden // SUB, SUB, LANES)
        spare = tile * (hidden // SUB)
        grads_ref[spare : spare + hidden // SUB, place : place + SUB, :] = part
    used = (flank.shape[1] // LANES) * (hidden // SUB)
    grads_ref[used:, place : place + SUB, :] = jnp.zeros((groups - used, SUB, LANES), F32)
    send_ref[...] = grads_ref[...].astype(BF16)
    rest = both_ref[:, rows * 2 * share :, :].astype(F32)
    tiles, place = gathered_rows(rest, 0, proj_in_ref.shape[1] // LANES, width)
    for tile, value in enumerate(tiles):
        proj_in_ref[:, tile * LANES : (tile + 1) * LANES] = value / residues
    tiles, place = gathered_rows(rest, place, 1, width)
    final_in_ref[...] = tiles[0] / residues
    tiles, place = gathered_rows(rest, place, 1, width)
    final_out_ref[...] = tiles[0] / residues


def msa_adjoint_kernel(
    sizes,
    parts_ref,
    left_grad_ref,
    msa_ref,
    msa_normal_ref,
    flank_t_ref,
    send_ref,
    adjoint_ref,
):
    rows, depth, hidden, groups = sizes
    half = hidden // 2
    own = rows * half
    summed = jnp.sum(parts_ref[...].astype(F32), axis=0).astype(BF16)
    right = summed[:own].astype(F32)
    flank = jnp.zeros((hidden, msa_normal_ref.shape[2]), F32)
    for row in range(rows):
        part = right[row * half : (row + 1) * half]
        right_grad = jnp.concatenate([part, pltpu.roll(part, LANES - depth, 1)], axis=0)[
            :, :depth
        ].astype(BF16)
        left_grad = left_grad_ref[row * hidden : (row + 1) * hidden, :depth]
        flank = flank + nn(right_grad, msa_normal_ref[row])
        grad = jnp.concatenate([left_grad, right_grad], axis=0)
        gradient = tn(grad, flank_t_ref[...])
        hatted, factor = moments(msa_ref[row].astype(F32), 1)
        adjoint_ref[row] = moments_adjoint(hatted, factor, gradient, 1).astype(BF16)
    rest = summed[own:]
    flank = flank.astype(BF16)
    for group in range(groups):
        send_ref[group, : rest.shape[0], :] = rest
        for tile in range(flank.shape[1] // LANES):
            at = rest.shape[0] + tile * hidden
            send_ref[group, at : at + hidden, :] = flank[:, tile * LANES : (tile + 1) * LANES]


def totals_kernel(sizes, parts_ref, proj_ref, final_ref, flank_ref, wide_ref):
    residues, hidden, groups, width = sizes
    parts = parts_ref[...].astype(F32)
    tiles, place = gathered_rows(parts, 0, proj_ref.shape[1] // LANES, width)
    for tile, value in enumerate(tiles):
        proj_ref[:, tile * LANES : (tile + 1) * LANES] = value / residues
    share = wide_ref.shape[0] // groups
    wide_ref[...] = parts[:, place : place + share, :].reshape(wide_ref.shape) / residues
    for c in range(hidden):
        final_ref[c * hidden : (c + 1) * hidden, :] = wide_ref[pl.ds(c, hidden, stride=hidden), :]
    place += share
    blocks = hidden // SUB
    for tile in range(flank_ref.shape[1] // LANES):
        lanes = slice(tile * LANES, (tile + 1) * LANES)
        left = parts[tile * blocks : (tile + 1) * blocks, place : place + SUB, :]
        flank_ref[:hidden, lanes] = left.reshape(hidden, LANES) / residues
        at = place + SUB + tile * hidden
        flank_ref[hidden:, lanes] = jnp.sum(parts[:, at : at + hidden, :], axis=0) / residues


def kernel_shards(
    edge_embedding,
    alignment_embedding,
    tensor_flank_matrix,
    tensor_final_matrix,
    outward_sigmoid_matrix,
    outward_final_matrix,
    inward_sigmoid_matrix,
    inward_final_matrix,
    adjoint_seed,
):
    groups = lax.axis_size("dap")
    rows, residues, width = edge_embedding.shape
    depth, _, features = alignment_embedding.shape
    hidden = tensor_flank_matrix.shape[1] // 2
    half = hidden // 2
    share = width // groups
    spots = rows * LANES
    square = hidden * hidden

    def shape(*dims, dtype=BF16):
        return jax.ShapeDtypeStruct(dims, dtype)

    msa = jnp.swapaxes(alignment_embedding, 0, 1)
    flank_t = tensor_flank_matrix.T
    send, msa_normal, left = launch(
        partial(msa_kernel, (rows, depth, hidden, groups)),
        [
            shape(groups, rows * half, LANES),
            shape(rows, depth, features),
            shape(2 * rows * hidden, LANES),
        ],
        (msa, flank_t),
        name="msa",
    )
    right = exchanged(send)

    final_sorted = (
        tensor_final_matrix.reshape(hidden, hidden, width).swapaxes(0, 1).reshape(square, width)
    )
    final_sorted_t = final_sorted.T
    gates_out_t = outward_sigmoid_matrix.T
    gates_in_t = inward_sigmoid_matrix.T
    final_out_t = outward_final_matrix.T
    final_in_t = inward_final_matrix.T

    send, spread, outer, pair_one = launch(
        partial(outer_kernel, (rows, residues, depth, hidden, groups, width)),
        [
            shape(groups, rows * 2 * share, LANES),
            shape(half * LANES, LANES),
            shape(square, spots),
            shape(width, spots),
        ],
        (right, left, edge_embedding, final_sorted_t, gates_out_t),
        [pltpu.VMEM((residues * half, LANES), F32)],
        name="outer",
    )

    def triangle(both, outgoing):
        return launch(
            partial(triangle_kernel, (residues, share), outgoing),
            [shape(groups, rows * share, LANES)],
            (both,),
            [
                pltpu.VMEM((residues * 2 * share, LANES), F32),
                pltpu.VMEM((residues * share, LANES), F32),
            ],
            name="triangle_out" if outgoing else "triangle_in",
        )[0]

    def triangle_adjoint(both, grads, outgoing):
        riders = grads.shape[1] - rows * share
        return launch(
            partial(triangle_adjoint_kernel, (residues, share, rows, riders), outgoing),
            [shape(groups, rows * 2 * share + riders, LANES)],
            (both, grads),
            [
                pltpu.VMEM((residues * 2 * share, LANES), F32),
                pltpu.VMEM((residues * share, LANES), F32),
                pltpu.VMEM((residues * 2 * share, LANES), F32),
            ],
            name="adjoint_out" if outgoing else "adjoint_in",
        )[0]

    both_out = exchanged(send)
    tri_out = exchanged(triangle(both_out, True))
    send, pair_two = launch(
        partial(middle_kernel, (rows, groups, width)),
        [shape(groups, rows * 2 * share, LANES), shape(width, spots)],
        (tri_out, pair_one, gates_out_t, final_out_t, gates_in_t),
        name="middle",
    )
    both_in = exchanged(send)
    tri_in = exchanged(triangle(both_in, False))
    send, updated, seed_t, grad_gate_in, final_in_sum = launch(
        partial(turn_kernel, (rows, residues, groups, width)),
        [
            shape(groups, rows * share, LANES),
            shape(rows, residues, width),
            shape(width, spots),
            shape(width, spots),
            shape(width, width, dtype=F32),
        ],
        (tri_in, pair_two, adjoint_seed, gates_in_t, inward_final_matrix, final_in_t),
        [
            pltpu.VMEM((groups, rows * share, LANES), F32),
            pltpu.VMEM((width, spots), BF16),
            pltpu.VMEM((width, spots), BF16),
        ],
        name="turn",
    )
    grads = exchanged(triangle_adjoint(both_in, exchanged(send), False))
    riders = share * (gates_in_t.shape[0] // LANES + 2)
    send, grad_two, grad_gate_out = launch(
        partial(between_kernel, (rows, groups, width)),
        [
            shape(groups, rows * share + riders, LANES),
            shape(width, spots, dtype=F32),
            shape(width, spots),
        ],
        (
            grads,
            pair_two,
            seed_t,
            grad_gate_in,
            gates_in_t,
            inward_sigmoid_matrix,
            final_in_sum,
            tri_out,
            pair_one,
            gates_out_t,
            outward_final_matrix,
            final_out_t,
        ),
        [
            pltpu.VMEM((groups, rows * share + riders, LANES), F32),
            pltpu.VMEM((width, spots), BF16),
            pltpu.VMEM((5 * width, spots), BF16),
            pltpu.VMEM((width, spots), BF16),
            pltpu.VMEM((width, spots), BF16),
        ],
        name="between",
    )
    grads = exchanged(triangle_adjoint(both_out, exchanged(send), True))
    count = rows * half + share * 5 + square // groups + SUB
    send, edge_adjoint, left_grad, proj_in, final_in, final_out = launch(
        partial(close_kernel, (rows, residues, depth, hidden, groups, width)),
        [
            shape(groups, count, LANES),
            shape(rows, residues, width),
            shape(rows * hidden, LANES),
            shape(width, 5 * width, dtype=F32),
            shape(width, width, dtype=F32),
            shape(width, width, dtype=F32),
        ],
        (
            grads,
            pair_one,
            grad_two,
            grad_gate_out,
            gates_out_t,
            outward_sigmoid_matrix,
            outer,
            final_sorted,
            spread,
            left,
            msa_normal,
        ),
        [
            pltpu.VMEM((groups, count, LANES), F32),
            pltpu.VMEM((width, spots), BF16),
            pltpu.VMEM((5 * width, spots), BF16),
            pltpu.VMEM((width, spots), BF16),
            pltpu.VMEM((2 * rows * hidden, half * LANES), BF16),
            pltpu.VMEM((residues * half, LANES), F32),
        ],
        name="close",
    )
    rest = count - rows * half
    send, msa_adjoint = launch(
        partial(msa_adjoint_kernel, (rows, depth, hidden, groups)),
        [
            shape(groups, rest + hidden * features // LANES, LANES),
            shape(rows, depth, features),
        ],
        (exchanged(send), left_grad, msa, msa_normal, flank_t),
        name="msa_adjoint",
    )
    proj_out, outer_final, outer_proj_t = launch(
        partial(totals_kernel, (residues, hidden, groups, width)),
        [
            shape(width, 5 * width, dtype=F32),
            shape(square, width, dtype=F32),
            shape(2 * hidden, features, dtype=F32),
        ],
        (exchanged(send),),
        [pltpu.VMEM((square, width), F32)],
        name="totals",
    )
    return (
        updated,
        edge_adjoint,
        jnp.swapaxes(msa_adjoint, 0, 1),
        outer_proj_t.T,
        outer_final,
        proj_out,
        final_out,
        proj_in,
        final_in,
    )


def any_shards(edge_embedding, alignment_embedding, tensor_flank_matrix, *others):
    groups = lax.axis_size("dap")
    rows, residues, width = edge_embedding.shape
    depth, _, features = alignment_embedding.shape
    hidden = tensor_flank_matrix.shape[1] // 2
    fits = (
        width == LANES
        and others[2].shape[0] == width
        and width % (groups * SUB) == 0
        and residues <= LANES
        and residues % SUB == 0
        and (rows * hidden // 2) % 16 == 0
        and (rows * width // groups) % 16 == 0
        and 2 * depth == LANES
        and hidden == 32
        and features % LANES == 0
        and (features // LANES) * (hidden // SUB) <= groups
        and hidden * hidden % (groups * SUB) == 0
    )
    program = kernel_shards if fits else shards
    return program(edge_embedding, alignment_embedding, tensor_flank_matrix, *others)


def solution(mesh):
    placed = (
        P(("dp", "dap"), None, None),
        P("dp", "dap", None),
        P(),
        P(),
        P(),
        P(),
        P(),
        P(),
        P(("dp", "dap"), None, None),
    )
    return jax.shard_map(
        any_shards,
        mesh=mesh,
        in_specs=placed,
        out_specs=(
            P(("dp", "dap"), None, None),
            P(("dp", "dap"), None, None),
            P("dp", "dap", None),
            P("dp", None),
            P("dp", None),
            P("dp", None),
            P("dp", None),
            P("dp", None),
            P("dp", None),
        ),
        check_vma=False,
    )
```

```python
from functools import partial

import jax
import jax.numpy as jnp
from jax import lax
from jax.experimental import pallas as pl
from jax.experimental.pallas import tpu as pltpu
from jax.sharding import PartitionSpec as P

EPSILON = 1e-05


def truncated_numbers(values):
    return lax.optimization_barrier(values.astype(jnp.bfloat16))


def edge_standardized(values, which_axis):
    average = jnp.mean(values, axis=which_axis, keepdims=True)
    centred = values - average
    factor = lax.rsqrt(jnp.mean(centred * centred, axis=which_axis, keepdims=True) + EPSILON)
    return centred * factor


def standardizer_adjoint(values, gradient, which_axis):
    average = jnp.mean(values, axis=which_axis, keepdims=True)
    centred = values - average
    factor = lax.rsqrt(jnp.mean(centred * centred, axis=which_axis, keepdims=True) + EPSILON)
    hatted = centred * factor
    return factor * (
        gradient
        - jnp.mean(gradient, axis=which_axis, keepdims=True)
        - hatted * jnp.mean(gradient * hatted, axis=which_axis, keepdims=True)
    )


def sigmoid_pieces(edge_entry, linear_mapping, latent_tensor):
    standardized_edges = truncated_numbers(edge_standardized(edge_entry.astype(jnp.float32), 2))
    gate_pre = jnp.dot(
        standardized_edges,
        linear_mapping[:, 4 * latent_tensor :],
        preferred_element_type=jnp.float32,
    )
    split_pre = jnp.einsum(
        "rnz,zc->crn",
        standardized_edges,
        linear_mapping[:, : 4 * latent_tensor],
        preferred_element_type=jnp.float32,
    )
    source_masked = truncated_numbers(
        jax.nn.sigmoid(split_pre[:latent_tensor]) * split_pre[latent_tensor : 2 * latent_tensor]
    )
    target_masked = truncated_numbers(
        jax.nn.sigmoid(split_pre[2 * latent_tensor : 3 * latent_tensor])
        * split_pre[3 * latent_tensor :]
    )
    return (standardized_edges, gate_pre, split_pre, source_masked, target_masked)


def grouped(values, groups):
    return values.reshape((groups, values.shape[0] // groups) + values.shape[1:])


def gathered(values, axis):
    groups = lax.axis_size("dap")
    copies = jnp.broadcast_to(values[None], (groups,) + values.shape)
    return jnp.moveaxis(lax.all_to_all(copies, "dap", 0, 0, tiled=True), 0, axis)


def exchanged(values):
    return lax.all_to_all(values, "dap", split_axis=0, concat_axis=0, tiled=True)


def totalled(parts):
    groups = lax.axis_size("dap")
    flat = jnp.concatenate([part.reshape(-1) for part in parts])
    unit = groups * 16 * 128
    padded = -(-flat.size // unit) * unit
    blocks = jnp.pad(flat, (0, padded - flat.size)).reshape(groups, -1, 128)
    mine = exchanged(truncated_numbers(blocks)).astype(jnp.float32).sum(axis=0)
    whole = gathered(truncated_numbers(mine), 0).astype(jnp.float32).reshape(-1)
    out, place = [], 0
    for part in parts:
        out.append(whole[place : place + part.size].reshape(part.shape))
        place += part.size
    return out


def to_channels(*rows):
    groups = lax.axis_size("dap")
    packed = jnp.stack([grouped(values, groups) for values in rows], axis=1)
    received = exchanged(packed)
    return [
        jnp.moveaxis(received[:, at], 0, 1).reshape(
            received.shape[2], -1, received.shape[4]
        )[None]
        for at in range(len(rows))
    ]


def to_rows(*columns):
    groups = lax.axis_size("dap")
    packed = jnp.stack(
        [
            jnp.moveaxis(
                values[0].reshape(values.shape[1], groups, -1, values.shape[3]), 1, 0
            )
            for values in columns
        ],
        axis=1,
    )
    received = exchanged(packed)
    return [
        received[:, at].reshape((-1,) + received.shape[3:]) for at in range(len(columns))
    ]


def contract_items(left_cols, right_cols, outgoing):
    if outgoing:
        return jnp.einsum(
            "xqik,xqjk->xqij", left_cols, right_cols, preferred_element_type=jnp.float32
        )
    return jnp.einsum("xqki,xqkj->xqij", left_cols, right_cols, preferred_element_type=jnp.float32)


def contract_back_items(grad_cols, left_cols, right_cols, outgoing):
    if outgoing:
        source_adjoint = jnp.einsum(
            "xqij,xqjk->xqik", grad_cols, right_cols, preferred_element_type=jnp.float32
        )
        target_adjoint = jnp.einsum(
            "xqij,xqik->xqjk", grad_cols, left_cols, preferred_element_type=jnp.float32
        )
    else:
        source_adjoint = jnp.einsum(
            "xqij,xqkj->xqki", grad_cols, right_cols, preferred_element_type=jnp.float32
        )
        target_adjoint = jnp.einsum(
            "xqij,xqki->xqkj", grad_cols, left_cols, preferred_element_type=jnp.float32
        )
    return (truncated_numbers(source_adjoint), truncated_numbers(target_adjoint))


def triangle_forward(edge_entry, linear_mapping, final, outgoing):
    latent_tensor = final.shape[0]
    groups = lax.axis_size("dap")
    standardized_edges, gate_pre, split_pre, source_masked, target_masked = sigmoid_pieces(
        edge_entry, linear_mapping, latent_tensor
    )
    kept = to_channels(source_masked, target_masked)
    triangle_cols = truncated_numbers(contract_items(kept[0], kept[1], outgoing))
    (triangle,) = to_rows(triangle_cols)
    unit_norm = truncated_numbers(edge_standardized(triangle.astype(jnp.float32), 0))
    values = jnp.einsum("crn,cz->rnz", unit_norm, final, preferred_element_type=jnp.float32)
    pair_new = truncated_numbers(edge_entry.astype(jnp.float32) + jax.nn.sigmoid(gate_pre) * values)
    return (pair_new, triangle, kept)


def triangle_back(edge_entry, linear_mapping, final, outgoing, triangle, kept, gradient):
    latent_tensor = final.shape[0]
    groups = lax.axis_size("dap")
    standardized_edges, gate_pre, split_pre, source_masked, target_masked = sigmoid_pieces(
        edge_entry, linear_mapping, latent_tensor
    )
    sigmoid_factor = jax.nn.sigmoid(gate_pre)
    tri_wide = triangle.astype(jnp.float32)
    unit_norm = truncated_numbers(edge_standardized(tri_wide, 0))
    values = jnp.einsum("crn,cz->rnz", unit_norm, final, preferred_element_type=jnp.float32)
    scaled = truncated_numbers(gradient * sigmoid_factor)
    final_sum = jnp.einsum("crn,rnz->cz", unit_norm, scaled, preferred_element_type=jnp.float32)
    grad_unit = jnp.einsum("rnz,cz->crn", scaled, final, preferred_element_type=jnp.float32)
    adjoint_sigmoid = truncated_numbers(gradient * values * sigmoid_factor * (1.0 - sigmoid_factor))
    grad_triangle = truncated_numbers(standardizer_adjoint(tri_wide, grad_unit, 0))
    (gradient_cols,) = to_channels(grad_triangle)
    left_back, right_back = contract_back_items(gradient_cols, kept[0], kept[1], outgoing)
    source_adjoint, target_adjoint = [
        values.astype(jnp.float32) for values in to_rows(left_back, right_back)
    ]
    logistic_primary = jax.nn.sigmoid(split_pre[:latent_tensor])
    logistic_tertiary = jax.nn.sigmoid(split_pre[2 * latent_tensor : 3 * latent_tensor])
    grad_split = truncated_numbers(
        jnp.concatenate(
            [
                source_adjoint
                * split_pre[latent_tensor : 2 * latent_tensor]
                * logistic_primary
                * (1.0 - logistic_primary),
                source_adjoint * logistic_primary,
                target_adjoint
                * split_pre[3 * latent_tensor :]
                * logistic_tertiary
                * (1.0 - logistic_tertiary),
                target_adjoint * logistic_tertiary,
            ],
            axis=0,
        )
    )
    proj_sum = jnp.concatenate(
        [
            jnp.einsum(
                "rnz,crn->zc", standardized_edges, grad_split, preferred_element_type=jnp.float32
            ),
            jnp.einsum(
                "rnz,rnc->zc",
                standardized_edges,
                adjoint_sigmoid,
                preferred_element_type=jnp.float32,
            ),
        ],
        axis=1,
    )
    grad_norm = jnp.einsum(
        "crn,zc->rnz",
        grad_split,
        linear_mapping[:, : 4 * latent_tensor],
        preferred_element_type=jnp.float32,
    )
    grad_norm = grad_norm + jnp.dot(
        adjoint_sigmoid,
        linear_mapping[:, 4 * latent_tensor :].T,
        preferred_element_type=jnp.float32,
    )
    grad_pair = gradient + standardizer_adjoint(edge_entry.astype(jnp.float32), grad_norm, 2)
    return (grad_pair, proj_sum, final_sum)


def shards(
    edge_embedding,
    alignment_embedding,
    tensor_flank_matrix,
    tensor_final_matrix,
    outward_sigmoid_matrix,
    outward_final_matrix,
    inward_sigmoid_matrix,
    inward_final_matrix,
    adjoint_seed,
):
    rows_here = edge_embedding.shape[0]
    residues = edge_embedding.shape[1]
    alignment_depth = alignment_embedding.shape[0]
    contraction_extent = tensor_flank_matrix.shape[1] // 2
    alignment_standardized = truncated_numbers(
        edge_standardized(alignment_embedding.astype(jnp.float32), 2)
    )
    alignment_mapped = jnp.dot(
        alignment_standardized, tensor_flank_matrix, preferred_element_type=jnp.float32
    )
    tensor_source_factor = truncated_numbers(alignment_mapped[..., :contraction_extent])
    tensor_target_factor = truncated_numbers(alignment_mapped[..., contraction_extent:])
    right_all = gathered(tensor_target_factor, 1).reshape(
        alignment_depth, residues, contraction_extent
    )
    tile_lines = 128 if residues % 128 == 0 else residues
    tile_number = residues // tile_lines
    outer_parts = []
    first_parts = []
    for block_index in range(tile_number):
        lower = block_index * tile_lines
        right_block = right_all[:, lower : lower + tile_lines]
        triangle_contraction = jnp.einsum(
            "sic,sjd->ijcd", tensor_source_factor, right_block, preferred_element_type=jnp.float32
        )
        outer_block = truncated_numbers(
            triangle_contraction.reshape(
                rows_here, tile_lines, contraction_extent * contraction_extent
            )
            / alignment_depth
        )
        update = jnp.dot(outer_block, tensor_final_matrix, preferred_element_type=jnp.float32)
        first_parts.append(
            truncated_numbers(
                edge_embedding[:, lower : lower + tile_lines].astype(jnp.float32) + update
            )
        )
        outer_parts.append(outer_block)
    outer_mean = jnp.concatenate(outer_parts, axis=1)
    pair_one = jnp.concatenate(first_parts, axis=1)
    pair_two, triangle_out, kept_out = triangle_forward(
        pair_one, outward_sigmoid_matrix, outward_final_matrix, True
    )
    edge_embedding_updated, triangle_in, kept_in = triangle_forward(
        pair_two, inward_sigmoid_matrix, inward_final_matrix, False
    )
    grad_two, inward_sigmoid_accrual, inward_final_accrual = triangle_back(
        pair_two,
        inward_sigmoid_matrix,
        inward_final_matrix,
        False,
        triangle_in,
        kept_in,
        adjoint_seed.astype(jnp.float32),
    )
    grad_one, outward_sigmoid_accrual, outward_final_accrual = triangle_back(
        pair_one, outward_sigmoid_matrix, outward_final_matrix, True, triangle_out, kept_out, grad_two
    )
    edge_embedding_adjoint = truncated_numbers(grad_one)
    tensor_final_accrual = jnp.einsum(
        "rnk,rnz->kz", outer_mean, edge_embedding_adjoint, preferred_element_type=jnp.float32
    )
    source_adjoint = jnp.zeros((alignment_depth, rows_here, contraction_extent), jnp.float32)
    outer_grads = []
    for block_index in range(tile_number):
        lower = block_index * tile_lines
        right_block = right_all[:, lower : lower + tile_lines]
        adjoint_tensor_mean = truncated_numbers(
            jnp.dot(
                edge_embedding_adjoint[:, lower : lower + tile_lines],
                tensor_final_matrix.T,
                preferred_element_type=jnp.float32,
            )
        )
        adjoint_tensor_mean = adjoint_tensor_mean.reshape(
            rows_here, tile_lines, contraction_extent, contraction_extent
        )
        source_adjoint = (
            source_adjoint
            + jnp.einsum(
                "mopz,loz->lmp",
                adjoint_tensor_mean,
                right_block,
                preferred_element_type=jnp.float32,
            )
            / alignment_depth
        )
        outer_grads.append(adjoint_tensor_mean)
    pair_columns = lax.all_to_all(
        edge_embedding_adjoint, "dap", split_axis=1, concat_axis=0, tiled=True
    )
    left_all = gathered(tensor_source_factor, 1).reshape(
        alignment_depth, residues, contraction_extent
    )
    target_adjoint = jnp.zeros((alignment_depth, rows_here, contraction_extent), jnp.float32)
    for block_index in range(tile_number):
        lower = block_index * tile_lines
        column_grad = truncated_numbers(
            jnp.dot(
                pair_columns[lower : lower + tile_lines],
                tensor_final_matrix.T,
                preferred_element_type=jnp.float32,
            )
        )
        column_grad = column_grad.reshape(
            tile_lines, rows_here, contraction_extent, contraction_extent
        )
        target_adjoint = (
            target_adjoint
            + jnp.einsum(
                "gxqp,vgq->vxp",
                column_grad,
                left_all[:, lower : lower + tile_lines],
                preferred_element_type=jnp.float32,
            )
            / alignment_depth
        )
    alignment_mapped_adjoint = truncated_numbers(
        jnp.concatenate([source_adjoint, target_adjoint], axis=2)
    )
    tensor_flank_accrual = jnp.einsum(
        "ajo,ajm->om",
        alignment_standardized,
        alignment_mapped_adjoint,
        preferred_element_type=jnp.float32,
    )
    alignment_standard_adjoint = jnp.dot(
        alignment_mapped_adjoint, tensor_flank_matrix.T, preferred_element_type=jnp.float32
    )
    alignment_adjoint = truncated_numbers(
        standardizer_adjoint(alignment_embedding.astype(jnp.float32), alignment_standard_adjoint, 2)
    )
    totals = totalled(
        (
            tensor_flank_accrual,
            tensor_final_accrual,
            outward_sigmoid_accrual,
            outward_final_accrual,
            inward_sigmoid_accrual,
            inward_final_accrual,
        )
    )
    return (
        edge_embedding_updated,
        edge_embedding_adjoint,
        alignment_adjoint,
        totals[0] / residues,
        totals[1] / residues,
        totals[2] / residues,
        totals[3] / residues,
        totals[4] / residues,
        totals[5] / residues,
    )


F32 = jnp.float32
BF16 = jnp.bfloat16
LANES = 128
SUB = 8


def nn(a, b):
    return lax.dot_general(a, b, (((1,), (0,)), ((), ())), preferred_element_type=F32)


def nt(a, b):
    return lax.dot_general(a, b, (((1,), (1,)), ((), ())), preferred_element_type=F32)


def tn(a, b):
    return lax.dot_general(a, b, (((0,), (0,)), ((), ())), preferred_element_type=F32)


def launch(body, outs, args, scratch=(), name=None, flops=2e8):
    vmem = pl.BlockSpec(memory_space=pltpu.VMEM)
    moved = sum(a.size * a.dtype.itemsize for a in args) + sum(
        o.size * o.dtype.itemsize for o in outs
    )
    return pl.pallas_call(
        body,
        out_shape=outs,
        in_specs=[vmem] * len(args),
        out_specs=[vmem] * len(outs),
        scratch_shapes=list(scratch),
        name=name,
        cost_estimate=pl.CostEstimate(
            flops=int(flops), bytes_accessed=int(moved), transcendentals=0
        ),
        compiler_params=pltpu.CompilerParams(vmem_limit_bytes=24 * 1024 * 1024),
    )(*args)


def moments(x, axis):
    average = jnp.mean(x, axis=axis, keepdims=True)
    centred = x - average
    factor = lax.rsqrt(jnp.mean(centred * centred, axis=axis, keepdims=True) + EPSILON)
    return centred * factor, factor


def moments_adjoint(hatted, factor, gradient, axis):
    return factor * (
        gradient
        - jnp.mean(gradient, axis=axis, keepdims=True)
        - hatted * jnp.mean(gradient * hatted, axis=axis, keepdims=True)
    )


def tall(x):
    return jnp.concatenate([x, jnp.zeros((LANES - x.shape[0], x.shape[1]), x.dtype)], axis=0)


def dealt(x, groups):
    return x.reshape((groups, x.shape[0] // groups) + x.shape[1:])


def gated_pair(projected, width):
    left = jax.nn.sigmoid(projected[:width]) * projected[width : 2 * width]
    right = jax.nn.sigmoid(projected[2 * width : 3 * width]) * projected[3 * width : 4 * width]
    return left, right


def send_pair(out_ref, row, left, right, groups):
    both = jnp.concatenate([dealt(left, groups), dealt(right, groups)], axis=1)
    wide = both.shape[1]
    out_ref[:, row * wide : (row + 1) * wide, :] = both.astype(BF16)


def msa_kernel(sizes, msa_ref, flank_t_ref, send_ref, normal_ref, left_ref):
    rows, depth, hidden, groups = sizes
    for row in range(rows):
        hatted, _ = moments(msa_ref[row].astype(F32), 1)
        normal = hatted.astype(BF16)
        normal_ref[row] = normal
        twice = jnp.concatenate([normal, normal], axis=0)
        mapped = nt(flank_t_ref[...], twice)
        lane = lax.broadcasted_iota(jnp.int32, (hidden, LANES), 1)
        low = lane < depth
        left = mapped[:hidden]
        left_ref[row * hidden : (row + 1) * hidden] = jnp.where(low, left, 0.0).astype(BF16)
        left_ref[(rows + row) * hidden : (rows + row + 1) * hidden] = jnp.where(
            low, 0.0, left
        ).astype(BF16)
        half = hidden // 2
        right = jnp.where(
            low[:half], mapped[hidden : hidden + half], mapped[hidden + half :]
        ).astype(BF16)
        for group in range(groups):
            send_ref[group, row * half : (row + 1) * half, :] = right


def outer_kernel(
    sizes,
    right_ref,
    left_ref,
    edge_ref,
    final_t_ref,
    gates_t_ref,
    send_ref,
    spread_ref,
    outer_ref,
    pair_ref,
    wide_ref,
):
    rows, residues, depth, hidden, groups, width = sizes
    half = hidden // 2
    wide_ref[...] = right_ref[...].reshape(wide_ref.shape).astype(F32)
    for d in range(half):
        picked = wide_ref[pl.ds(d, residues, stride=half), :]
        spread_ref[d * LANES : (d + 1) * LANES, :] = tall(picked).astype(BF16)
    for d in range(0, half, 2):
        block = nt(left_ref[...], spread_ref[d * LANES : (d + 2) * LANES, :]) / depth
        for e in range(2):
            for h in range(2):
                for row in range(rows):
                    at = (h * rows + row) * hidden
                    to = (h * half + d + e) * hidden
                    outer_ref[to : to + hidden, row * LANES : (row + 1) * LANES] = block[
                        at : at + hidden, e * LANES : (e + 1) * LANES
                    ].astype(BF16)
    update = nn(final_t_ref[...], outer_ref[...])
    for row in range(rows):
        lanes = slice(row * LANES, (row + 1) * LANES)
        entry = tall(edge_ref[row].astype(F32)).T
        pair = (entry + update[:, lanes]).astype(BF16)
        pair_ref[:, lanes] = pair
        hatted, _ = moments(pair.astype(F32), 0)
        projected = nn(gates_t_ref[: 4 * width, :], hatted.astype(BF16))
        left, right = gated_pair(projected, width)
        send_pair(send_ref, row, left, right, groups)


def triangle_kernel(sizes, outgoing, both_ref, send_ref, wide_ref, result_ref):
    residues, share = sizes
    wide_ref[...] = both_ref[...].reshape(wide_ref.shape).astype(F32)
    for c in range(share):
        left = wide_ref[pl.ds(c, residues, stride=2 * share), :].astype(BF16)
        right = wide_ref[pl.ds(share + c, residues, stride=2 * share), :].astype(BF16)
        if outgoing:
            product = nt(left, tall(right))
        else:
            product = tn(left, right)[:residues]
        result_ref[pl.ds(c, residues, stride=share), :] = product
    send_ref[...] = result_ref[...].astype(BF16).reshape(send_ref.shape)


def triangle_adjoint_kernel(
    sizes, outgoing, both_ref, grad_ref, send_ref, wide_ref, tri_ref, result_ref
):
    residues, share, rows, riders = sizes
    own = rows * share
    wide_ref[...] = both_ref[...].reshape(wide_ref.shape).astype(F32)
    tri_ref[...] = grad_ref[:, :own, :].astype(F32).reshape(tri_ref.shape)
    for c in range(share):
        left = wide_ref[pl.ds(c, residues, stride=2 * share), :].astype(BF16)
        right = wide_ref[pl.ds(share + c, residues, stride=2 * share), :].astype(BF16)
        grad = tri_ref[pl.ds(c, residues, stride=share), :].astype(BF16)
        if outgoing:
            grad_left = nn(grad, tall(right))
            grad_right = tn(grad, left)[:residues]
        else:
            grad_left = nt(right, tall(grad))
            grad_right = nn(left, tall(grad))
        result_ref[pl.ds(c, residues, stride=2 * share), :] = grad_left
        result_ref[pl.ds(share + c, residues, stride=2 * share), :] = grad_right
    groups = send_ref.shape[0]
    send_ref[:, : 2 * own, :] = (
        result_ref[...].astype(BF16).reshape(groups, 2 * own, LANES)
    )
    if riders:
        summed = jnp.sum(grad_ref[:, own:, :].astype(F32), axis=0).astype(BF16)
        for group in range(groups):
            send_ref[group, 2 * own :, :] = summed


def middle_kernel(
    sizes,
    tri_ref,
    pair_ref,
    gates_t_ref,
    final_t_ref,
    next_gates_t_ref,
    send_ref,
    next_ref,
):
    rows, groups, width = sizes
    share = width // groups
    received = tri_ref[...].astype(F32)
    for row in range(rows):
        lanes = slice(row * LANES, (row + 1) * LANES)
        tri = received[:, row * share : (row + 1) * share, :].reshape(width, LANES)
        unit, _ = moments(tri, 0)
        values = nn(final_t_ref[...], unit.astype(BF16))
        pair = pair_ref[:, lanes].astype(F32)
        hatted, _ = moments(pair, 0)
        gate = jax.nn.sigmoid(nn(gates_t_ref[4 * width :, :], hatted.astype(BF16)))
        following = (pair + gate * values).astype(BF16)
        next_ref[:, lanes] = following
        hatted, _ = moments(following.astype(F32), 0)
        projected = nn(next_gates_t_ref[: 4 * width, :], hatted.astype(BF16))
        left, right = gated_pair(projected, width)
        send_pair(send_ref, row, left, right, groups)


def tri_adjoint_row(tri, pair, gradient, gates_t_ref, final_ref, final_t_ref, width):
    hatted_tri, factor = moments(tri, 0)
    unit = hatted_tri.astype(BF16)
    values = nn(final_t_ref[...], unit)
    hatted, _ = moments(pair, 0)
    gate = jax.nn.sigmoid(nn(gates_t_ref[4 * width :, :], hatted.astype(BF16)))
    scaled = (gradient * gate).astype(BF16)
    grad_unit = nn(final_ref[...], scaled)
    grad_tri = moments_adjoint(hatted_tri, factor, grad_unit, 0)
    grad_gate = (gradient * values * gate * (1.0 - gate)).astype(BF16)
    return unit, scaled, values, gate, grad_tri, grad_gate


def turn_kernel(
    sizes,
    tri_ref,
    pair_ref,
    seed_ref,
    gates_t_ref,
    final_ref,
    final_t_ref,
    send_ref,
    out_ref,
    seed_t_ref,
    grad_gate_ref,
    final_sum_ref,
    grads_ref,
    unit_ref,
    scaled_ref,
):
    rows, residues, groups, width = sizes
    share = width // groups
    received = tri_ref[...].astype(F32)
    for row in range(rows):
        lanes = slice(row * LANES, (row + 1) * LANES)
        tri = received[:, row * share : (row + 1) * share, :].reshape(width, LANES)
        pair = pair_ref[:, lanes].astype(F32)
        gradient = tall(seed_ref[row].astype(F32)).T
        seed_t_ref[:, lanes] = gradient.astype(BF16)
        unit, scaled, values, gate, grad_tri, grad_gate = tri_adjoint_row(
            tri, pair, gradient, gates_t_ref, final_ref, final_t_ref, width
        )
        unit_ref[:, lanes] = unit
        scaled_ref[:, lanes] = scaled
        grad_gate_ref[:, lanes] = grad_gate
        grads_ref[:, row * share : (row + 1) * share, :] = dealt(grad_tri, groups)
        out_ref[row] = (pair + gate * values).T[:residues].astype(BF16)
    send_ref[...] = grads_ref[...].astype(BF16)
    final_sum_ref[...] = nt(unit_ref[...], scaled_ref[...])


def proj_adjoint_row(row, received, pair, grad_gate, gates_t_ref, gates_ref, normal_ref, proj_ref, width):
    share2 = received.shape[1]
    lanes = slice(row * LANES, (row + 1) * LANES)
    grad_left = received[:, : share2 // 2, :].reshape(width, LANES)
    grad_right = received[:, share2 // 2 :, :].reshape(width, LANES)
    hatted, factor = moments(pair, 0)
    normal = hatted.astype(BF16)
    normal_ref[:, lanes] = normal
    projected = nn(gates_t_ref[: 4 * width, :], normal)
    first = jax.nn.sigmoid(projected[:width])
    third = jax.nn.sigmoid(projected[2 * width : 3 * width])
    left_part = grad_left * first
    right_part = grad_right * third
    proj_ref[:width, lanes] = (
        left_part * projected[width : 2 * width] * (1.0 - first)
    ).astype(BF16)
    proj_ref[width : 2 * width, lanes] = left_part.astype(BF16)
    proj_ref[2 * width : 3 * width, lanes] = (
        right_part * projected[3 * width :] * (1.0 - third)
    ).astype(BF16)
    proj_ref[3 * width : 4 * width, lanes] = right_part.astype(BF16)
    proj_ref[4 * width :, lanes] = grad_gate
    grad_normal = nn(gates_ref[...], proj_ref[:, lanes])
    return moments_adjoint(hatted, factor, grad_normal, 0)


def deal_rows(out_ref, start, total, groups):
    for tile in range(total.shape[1] // LANES):
        block = dealt(total[:, tile * LANES : (tile + 1) * LANES], groups)
        out_ref[:, start : start + block.shape[1], :] = block
        start += block.shape[1]
    return start


def between_kernel(
    sizes,
    both_ref,
    pair_in_ref,
    seed_ref,
    grad_gate_in_ref,
    gates_in_t_ref,
    gates_in_ref,
    final_in_sum_ref,
    tri_ref,
    pair_out_ref,
    gates_out_t_ref,
    final_out_ref,
    final_out_t_ref,
    send_ref,
    grad_ref,
    grad_gate_ref,
    grads_ref,
    normal_ref,
    proj_ref,
    unit_ref,
    scaled_ref,
):
    rows, groups, width = sizes
    share = width // groups
    received = tri_ref[...].astype(F32)
    for row in range(rows):
        lanes = slice(row * LANES, (row + 1) * LANES)
        pair = pair_in_ref[:, lanes].astype(F32)
        both = both_ref[:, row * 2 * share : (row + 1) * 2 * share, :].astype(F32)
        gradient = seed_ref[:, lanes].astype(F32) + proj_adjoint_row(
            row,
            both,
            pair,
            grad_gate_in_ref[:, lanes],
            gates_in_t_ref,
            gates_in_ref,
            normal_ref,
            proj_ref,
            width,
        )
        grad_ref[:, lanes] = gradient
        tri = received[:, row * share : (row + 1) * share, :].reshape(width, LANES)
        unit, scaled, _, _, grad_tri, grad_gate = tri_adjoint_row(
            tri,
            pair_out_ref[:, lanes].astype(F32),
            gradient,
            gates_out_t_ref,
            final_out_ref,
            final_out_t_ref,
            width,
        )
        unit_ref[:, lanes] = unit
        scaled_ref[:, lanes] = scaled
        grad_gate_ref[:, lanes] = grad_gate
        grads_ref[:, row * share : (row + 1) * share, :] = dealt(grad_tri, groups)
    place = rows * share
    place = deal_rows(grads_ref, place, nt(normal_ref[...], proj_ref[...]), groups)
    place = deal_rows(grads_ref, place, final_in_sum_ref[...], groups)
    deal_rows(grads_ref, place, nt(unit_ref[...], scaled_ref[...]), groups)
    send_ref[...] = grads_ref[...].astype(BF16)


def gathered_rows(rest, start, tiles, width):
    out = []
    share = width // rest.shape[0]
    for tile in range(tiles):
        out.append(rest[:, start + tile * share : start + (tile + 1) * share, :].reshape(width, LANES))
    return out, start + tiles * share


def close_kernel(
    sizes,
    both_ref,
    pair_ref,
    grad_ref,
    grad_gate_ref,
    gates_t_ref,
    gates_ref,
    outer_ref,
    final_ref,
    spread_ref,
    left_ref,
    msa_normal_ref,
    send_ref,
    adjoint_ref,
    left_grad_ref,
    proj_in_ref,
    final_in_ref,
    final_out_ref,
    grads_ref,
    normal_ref,
    proj_ref,
    adjoint_t_ref,
    outer_grad_ref,
    right_grad_ref,
):
    rows, residues, depth, hidden, groups, width = sizes
    share = width // groups
    half = hidden // 2
    for row in range(rows):
        lanes = slice(row * LANES, (row + 1) * LANES)
        both = both_ref[:, row * 2 * share : (row + 1) * 2 * share, :].astype(F32)
        gradient = grad_ref[:, lanes] + proj_adjoint_row(
            row,
            both,
            pair_ref[:, lanes].astype(F32),
            grad_gate_ref[:, lanes],
            gates_t_ref,
            gates_ref,
            normal_ref,
            proj_ref,
            width,
        )
        adjoint = gradient.astype(BF16)
        adjoint_t_ref[:, lanes] = adjoint
        adjoint_ref[row] = adjoint.astype(F32).T[:residues].astype(BF16)
        spread_grad = nn(final_ref[...], adjoint).astype(BF16)
        for h in range(2):
            for d in range(half):
                at = (h * half + d) * hidden
                to = (h * rows + row) * hidden
                outer_grad_ref[to : to + hidden, d * LANES : (d + 1) * LANES] = spread_grad[
                    at : at + hidden
                ]
    for d in range(half):
        piece = tn(outer_grad_ref[:, d * LANES : (d + 1) * LANES], left_ref[...]) / depth
        right_grad_ref[pl.ds(d, residues, stride=half), :] = piece[:residues]
    own = rows * half
    grads_ref[:, :own, :] = right_grad_ref[...].reshape(groups, own, LANES)
    place = deal_rows(grads_ref, own, nt(normal_ref[...], proj_ref[...]), groups)
    outer_sum = nt(outer_ref[...], adjoint_t_ref[...])
    place = deal_rows(grads_ref, place, outer_sum, groups)
    stacked = nn(outer_grad_ref[...], spread_ref[...]) / depth
    count = rows * hidden
    lane = lax.broadcasted_iota(jnp.int32, (count, LANES), 1)
    left_grad = jnp.where(
        lane < depth, stacked[:count] + pltpu.roll(stacked[count:], LANES - depth, 1), 0.0
    ).astype(BF16)
    left_grad_ref[...] = left_grad
    flank = jnp.zeros((hidden, msa_normal_ref.shape[2]), F32)
    for row in range(rows):
        flank = flank + nn(
            left_grad[row * hidden : (row + 1) * hidden, :depth], msa_normal_ref[row]
        )
    for tile in range(flank.shape[1] // LANES):
        part = flank[:, tile * LANES : (tile + 1) * LANES].reshape(hidden // SUB, SUB, LANES)
        spare = tile * (hidden // SUB)
        grads_ref[spare : spare + hidden // SUB, place : place + SUB, :] = part
    used = (flank.shape[1] // LANES) * (hidden // SUB)
    grads_ref[used:, place : place + SUB, :] = jnp.zeros((groups - used, SUB, LANES), F32)
    send_ref[...] = grads_ref[...].astype(BF16)
    rest = both_ref[:, rows * 2 * share :, :].astype(F32)
    tiles, place = gathered_rows(rest, 0, proj_in_ref.shape[1] // LANES, width)
    for tile, value in enumerate(tiles):
        proj_in_ref[:, tile * LANES : (tile + 1) * LANES] = value / residues
    tiles, place = gathered_rows(rest, place, 1, width)
    final_in_ref[...] = tiles[0] / residues
    tiles, place = gathered_rows(rest, place, 1, width)
    final_out_ref[...] = tiles[0] / residues


def msa_adjoint_kernel(
    sizes,
    parts_ref,
    left_grad_ref,
    msa_ref,
    msa_normal_ref,
    flank_t_ref,
    send_ref,
    adjoint_ref,
):
    rows, depth, hidden, groups = sizes
    half = hidden // 2
    own = rows * half
    summed = jnp.sum(parts_ref[...].astype(F32), axis=0).astype(BF16)
    right = summed[:own].astype(F32)
    flank = jnp.zeros((hidden, msa_normal_ref.shape[2]), F32)
    for row in range(rows):
        part = right[row * half : (row + 1) * half]
        right_grad = jnp.concatenate([part, pltpu.roll(part, LANES - depth, 1)], axis=0)[
            :, :depth
        ].astype(BF16)
        left_grad = left_grad_ref[row * hidden : (row + 1) * hidden, :depth]
        flank = flank + nn(right_grad, msa_normal_ref[row])
        grad = jnp.concatenate([left_grad, right_grad], axis=0)
        gradient = tn(grad, flank_t_ref[...])
        hatted, factor = moments(msa_ref[row].astype(F32), 1)
        adjoint_ref[row] = moments_adjoint(hatted, factor, gradient, 1).astype(BF16)
    rest = summed[own:]
    flank = flank.astype(BF16)
    for group in range(groups):
        send_ref[group, : rest.shape[0], :] = rest
        for tile in range(flank.shape[1] // LANES):
            at = rest.shape[0] + tile * hidden
            send_ref[group, at : at + hidden, :] = flank[:, tile * LANES : (tile + 1) * LANES]


def totals_kernel(sizes, parts_ref, proj_ref, final_ref, flank_ref, wide_ref):
    residues, hidden, groups, width = sizes
    parts = parts_ref[...].astype(F32)
    tiles, place = gathered_rows(parts, 0, proj_ref.shape[1] // LANES, width)
    for tile, value in enumerate(tiles):
        proj_ref[:, tile * LANES : (tile + 1) * LANES] = value / residues
    share = wide_ref.shape[0] // groups
    wide_ref[...] = parts[:, place : place + share, :].reshape(wide_ref.shape) / residues
    for c in range(hidden):
        final_ref[c * hidden : (c + 1) * hidden, :] = wide_ref[pl.ds(c, hidden, stride=hidden), :]
    place += share
    blocks = hidden // SUB
    for tile in range(flank_ref.shape[1] // LANES):
        lanes = slice(tile * LANES, (tile + 1) * LANES)
        left = parts[tile * blocks : (tile + 1) * blocks, place : place + SUB, :]
        flank_ref[:hidden, lanes] = left.reshape(hidden, LANES) / residues
        at = place + SUB + tile * hidden
        flank_ref[hidden:, lanes] = jnp.sum(parts[:, at : at + hidden, :], axis=0) / residues


def kernel_shards(
    edge_embedding,
    alignment_embedding,
    tensor_flank_matrix,
    tensor_final_matrix,
    outward_sigmoid_matrix,
    outward_final_matrix,
    inward_sigmoid_matrix,
    inward_final_matrix,
    adjoint_seed,
):
    groups = lax.axis_size("dap")
    rows, residues, width = edge_embedding.shape
    depth, _, features = alignment_embedding.shape
    hidden = tensor_flank_matrix.shape[1] // 2
    half = hidden // 2
    share = width // groups
    spots = rows * LANES
    square = hidden * hidden

    def shape(*dims, dtype=BF16):
        return jax.ShapeDtypeStruct(dims, dtype)

    msa = jnp.swapaxes(alignment_embedding, 0, 1)
    flank_t = tensor_flank_matrix.T
    send, msa_normal, left = launch(
        partial(msa_kernel, (rows, depth, hidden, groups)),
        [
            shape(groups, rows * half, LANES),
            shape(rows, depth, features),
            shape(2 * rows * hidden, LANES),
        ],
        (msa, flank_t),
        name="msa",
    )
    right = exchanged(send)

    final_sorted = (
        tensor_final_matrix.reshape(hidden, hidden, width).swapaxes(0, 1).reshape(square, width)
    )
    final_sorted_t = final_sorted.T
    gates_out_t = outward_sigmoid_matrix.T
    gates_in_t = inward_sigmoid_matrix.T
    final_out_t = outward_final_matrix.T
    final_in_t = inward_final_matrix.T
    right, final_sorted, final_sorted_t, gates_out_t, gates_in_t, final_out_t, final_in_t = (
        lax.optimization_barrier(
            (right, final_sorted, final_sorted_t, gates_out_t, gates_in_t, final_out_t, final_in_t)
        )
    )

    send, spread, outer, pair_one = launch(
        partial(outer_kernel, (rows, residues, depth, hidden, groups, width)),
        [
            shape(groups, rows * 2 * share, LANES),
            shape(half * LANES, LANES),
            shape(square, spots),
            shape(width, spots),
        ],
        (right, left, edge_embedding, final_sorted_t, gates_out_t),
        [pltpu.VMEM((residues * half, LANES), F32)],
        name="outer",
    )

    def triangle(both, outgoing):
        return launch(
            partial(triangle_kernel, (residues, share), outgoing),
            [shape(groups, rows * share, LANES)],
            (both,),
            [
                pltpu.VMEM((residues * 2 * share, LANES), F32),
                pltpu.VMEM((residues * share, LANES), F32),
            ],
            name="triangle_out" if outgoing else "triangle_in",
        )[0]

    def triangle_adjoint(both, grads, outgoing):
        riders = grads.shape[1] - rows * share
        return launch(
            partial(triangle_adjoint_kernel, (residues, share, rows, riders), outgoing),
            [shape(groups, rows * 2 * share + riders, LANES)],
            (both, grads),
            [
                pltpu.VMEM((residues * 2 * share, LANES), F32),
                pltpu.VMEM((residues * share, LANES), F32),
                pltpu.VMEM((residues * 2 * share, LANES), F32),
            ],
            name="adjoint_out" if outgoing else "adjoint_in",
        )[0]

    both_out = exchanged(send)
    tri_out = exchanged(triangle(both_out, True))
    send, pair_two = launch(
        partial(middle_kernel, (rows, groups, width)),
        [shape(groups, rows * 2 * share, LANES), shape(width, spots)],
        (tri_out, pair_one, gates_out_t, final_out_t, gates_in_t),
        name="middle",
    )
    both_in = exchanged(send)
    tri_in = exchanged(triangle(both_in, False))
    send, updated, seed_t, grad_gate_in, final_in_sum = launch(
        partial(turn_kernel, (rows, residues, groups, width)),
        [
            shape(groups, rows * share, LANES),
            shape(rows, residues, width),
            shape(width, spots),
            shape(width, spots),
            shape(width, width, dtype=F32),
        ],
        (tri_in, pair_two, adjoint_seed, gates_in_t, inward_final_matrix, final_in_t),
        [
            pltpu.VMEM((groups, rows * share, LANES), F32),
            pltpu.VMEM((width, spots), BF16),
            pltpu.VMEM((width, spots), BF16),
        ],
        name="turn",
    )
    grads = exchanged(triangle_adjoint(both_in, exchanged(send), False))
    riders = share * (gates_in_t.shape[0] // LANES + 2)
    send, grad_two, grad_gate_out = launch(
        partial(between_kernel, (rows, groups, width)),
        [
            shape(groups, rows * share + riders, LANES),
            shape(width, spots, dtype=F32),
            shape(width, spots),
        ],
        (
            grads,
            pair_two,
            seed_t,
            grad_gate_in,
            gates_in_t,
            inward_sigmoid_matrix,
            final_in_sum,
            tri_out,
            pair_one,
            gates_out_t,
            outward_final_matrix,
            final_out_t,
        ),
        [
            pltpu.VMEM((groups, rows * share + riders, LANES), F32),
            pltpu.VMEM((width, spots), BF16),
            pltpu.VMEM((5 * width, spots), BF16),
            pltpu.VMEM((width, spots), BF16),
            pltpu.VMEM((width, spots), BF16),
        ],
        name="between",
    )
    grads = exchanged(triangle_adjoint(both_out, exchanged(send), True))
    count = rows * half + share * 5 + square // groups + SUB
    send, edge_adjoint, left_grad, proj_in, final_in, final_out = launch(
        partial(close_kernel, (rows, residues, depth, hidden, groups, width)),
        [
            shape(groups, count, LANES),
            shape(rows, residues, width),
            shape(rows * hidden, LANES),
            shape(width, 5 * width, dtype=F32),
            shape(width, width, dtype=F32),
            shape(width, width, dtype=F32),
        ],
        (
            grads,
            pair_one,
            grad_two,
            grad_gate_out,
            gates_out_t,
            outward_sigmoid_matrix,
            outer,
            final_sorted,
            spread,
            left,
            msa_normal,
        ),
        [
            pltpu.VMEM((groups, count, LANES), F32),
            pltpu.VMEM((width, spots), BF16),
            pltpu.VMEM((5 * width, spots), BF16),
            pltpu.VMEM((width, spots), BF16),
            pltpu.VMEM((2 * rows * hidden, half * LANES), BF16),
            pltpu.VMEM((residues * half, LANES), F32),
        ],
        name="close",
    )
    rest = count - rows * half
    send, msa_adjoint = launch(
        partial(msa_adjoint_kernel, (rows, depth, hidden, groups)),
        [
            shape(groups, rest + hidden * features // LANES, LANES),
            shape(rows, depth, features),
        ],
        (exchanged(send), left_grad, msa, msa_normal, flank_t),
        name="msa_adjoint",
    )
    proj_out, outer_final, outer_proj_t = launch(
        partial(totals_kernel, (residues, hidden, groups, width)),
        [
            shape(width, 5 * width, dtype=F32),
            shape(square, width, dtype=F32),
            shape(2 * hidden, features, dtype=F32),
        ],
        (exchanged(send),),
        [pltpu.VMEM((square, width), F32)],
        name="totals",
    )
    return (
        updated,
        edge_adjoint,
        jnp.swapaxes(msa_adjoint, 0, 1),
        outer_proj_t.T,
        outer_final,
        proj_out,
        final_out,
        proj_in,
        final_in,
    )


def any_shards(edge_embedding, alignment_embedding, tensor_flank_matrix, *others):
    groups = lax.axis_size("dap")
    rows, residues, width = edge_embedding.shape
    depth, _, features = alignment_embedding.shape
    hidden = tensor_flank_matrix.shape[1] // 2
    fits = (
        width == LANES
        and others[2].shape[0] == width
        and width % (groups * SUB) == 0
        and residues <= LANES
        and residues % SUB == 0
        and (rows * hidden // 2) % 16 == 0
        and (rows * width // groups) % 16 == 0
        and 2 * depth == LANES
        and hidden == 32
        and features % LANES == 0
        and (features // LANES) * (hidden // SUB) <= groups
        and hidden * hidden % (groups * SUB) == 0
    )
    program = kernel_shards if fits else shards
    return program(edge_embedding, alignment_embedding, tensor_flank_matrix, *others)


def solution(mesh):
    placed = (
        P(("dp", "dap"), None, None),
        P("dp", "dap", None),
        P(),
        P(),
        P(),
        P(),
        P(),
        P(),
        P(("dp", "dap"), None, None),
    )
    return jax.shard_map(
        any_shards,
        mesh=mesh,
        in_specs=placed,
        out_specs=(
            P(("dp", "dap"), None, None),
            P(("dp", "dap"), None, None),
            P("dp", "dap", None),
            P("dp", None),
            P("dp", None),
            P("dp", None),
            P("dp", None),
            P("dp", None),
            P("dp", None),
        ),
        check_vma=False,
    )
```

```python
from functools import partial

import jax
import jax.numpy as jnp
from jax import lax
from jax.experimental import pallas as pl
from jax.experimental.pallas import tpu as pltpu
from jax.sharding import PartitionSpec as P

EPSILON = 1e-05


def truncated_numbers(values):
    return lax.optimization_barrier(values.astype(jnp.bfloat16))


def edge_standardized(values, which_axis):
    average = jnp.mean(values, axis=which_axis, keepdims=True)
    centred = values - average
    factor = lax.rsqrt(jnp.mean(centred * centred, axis=which_axis, keepdims=True) + EPSILON)
    return centred * factor


def standardizer_adjoint(values, gradient, which_axis):
    average = jnp.mean(values, axis=which_axis, keepdims=True)
    centred = values - average
    factor = lax.rsqrt(jnp.mean(centred * centred, axis=which_axis, keepdims=True) + EPSILON)
    hatted = centred * factor
    return factor * (
        gradient
        - jnp.mean(gradient, axis=which_axis, keepdims=True)
        - hatted * jnp.mean(gradient * hatted, axis=which_axis, keepdims=True)
    )


def sigmoid_pieces(edge_entry, linear_mapping, latent_tensor):
    standardized_edges = truncated_numbers(edge_standardized(edge_entry.astype(jnp.float32), 2))
    gate_pre = jnp.dot(
        standardized_edges,
        linear_mapping[:, 4 * latent_tensor :],
        preferred_element_type=jnp.float32,
    )
    split_pre = jnp.einsum(
        "rnz,zc->crn",
        standardized_edges,
        linear_mapping[:, : 4 * latent_tensor],
        preferred_element_type=jnp.float32,
    )
    source_masked = truncated_numbers(
        jax.nn.sigmoid(split_pre[:latent_tensor]) * split_pre[latent_tensor : 2 * latent_tensor]
    )
    target_masked = truncated_numbers(
        jax.nn.sigmoid(split_pre[2 * latent_tensor : 3 * latent_tensor])
        * split_pre[3 * latent_tensor :]
    )
    return (standardized_edges, gate_pre, split_pre, source_masked, target_masked)


def grouped(values, groups):
    return values.reshape((groups, values.shape[0] // groups) + values.shape[1:])


def gathered(values, axis):
    groups = lax.axis_size("dap")
    copies = jnp.broadcast_to(values[None], (groups,) + values.shape)
    return jnp.moveaxis(lax.all_to_all(copies, "dap", 0, 0, tiled=True), 0, axis)


def exchanged(values):
    return lax.all_to_all(values, "dap", split_axis=0, concat_axis=0, tiled=True)


def totalled(parts):
    groups = lax.axis_size("dap")
    flat = jnp.concatenate([part.reshape(-1) for part in parts])
    unit = groups * 16 * 128
    padded = -(-flat.size // unit) * unit
    blocks = jnp.pad(flat, (0, padded - flat.size)).reshape(groups, -1, 128)
    mine = exchanged(truncated_numbers(blocks)).astype(jnp.float32).sum(axis=0)
    whole = gathered(truncated_numbers(mine), 0).astype(jnp.float32).reshape(-1)
    out, place = [], 0
    for part in parts:
        out.append(whole[place : place + part.size].reshape(part.shape))
        place += part.size
    return out


def to_channels(*rows):
    groups = lax.axis_size("dap")
    packed = jnp.stack([grouped(values, groups) for values in rows], axis=1)
    received = exchanged(packed)
    return [
        jnp.moveaxis(received[:, at], 0, 1).reshape(
            received.shape[2], -1, received.shape[4]
        )[None]
        for at in range(len(rows))
    ]


def to_rows(*columns):
    groups = lax.axis_size("dap")
    packed = jnp.stack(
        [
            jnp.moveaxis(
                values[0].reshape(values.shape[1], groups, -1, values.shape[3]), 1, 0
            )
            for values in columns
        ],
        axis=1,
    )
    received = exchanged(packed)
    return [
        received[:, at].reshape((-1,) + received.shape[3:]) for at in range(len(columns))
    ]


def contract_items(left_cols, right_cols, outgoing):
    if outgoing:
        return jnp.einsum(
            "xqik,xqjk->xqij", left_cols, right_cols, preferred_element_type=jnp.float32
        )
    return jnp.einsum("xqki,xqkj->xqij", left_cols, right_cols, preferred_element_type=jnp.float32)


def contract_back_items(grad_cols, left_cols, right_cols, outgoing):
    if outgoing:
        source_adjoint = jnp.einsum(
            "xqij,xqjk->xqik", grad_cols, right_cols, preferred_element_type=jnp.float32
        )
        target_adjoint = jnp.einsum(
            "xqij,xqik->xqjk", grad_cols, left_cols, preferred_element_type=jnp.float32
        )
    else:
        source_adjoint = jnp.einsum(
            "xqij,xqkj->xqki", grad_cols, right_cols, preferred_element_type=jnp.float32
        )
        target_adjoint = jnp.einsum(
            "xqij,xqki->xqkj", grad_cols, left_cols, preferred_element_type=jnp.float32
        )
    return (truncated_numbers(source_adjoint), truncated_numbers(target_adjoint))


def triangle_forward(edge_entry, linear_mapping, final, outgoing):
    latent_tensor = final.shape[0]
    groups = lax.axis_size("dap")
    standardized_edges, gate_pre, split_pre, source_masked, target_masked = sigmoid_pieces(
        edge_entry, linear_mapping, latent_tensor
    )
    kept = to_channels(source_masked, target_masked)
    triangle_cols = truncated_numbers(contract_items(kept[0], kept[1], outgoing))
    (triangle,) = to_rows(triangle_cols)
    unit_norm = truncated_numbers(edge_standardized(triangle.astype(jnp.float32), 0))
    values = jnp.einsum("crn,cz->rnz", unit_norm, final, preferred_element_type=jnp.float32)
    pair_new = truncated_numbers(edge_entry.astype(jnp.float32) + jax.nn.sigmoid(gate_pre) * values)
    return (pair_new, triangle, kept)


def triangle_back(edge_entry, linear_mapping, final, outgoing, triangle, kept, gradient):
    latent_tensor = final.shape[0]
    groups = lax.axis_size("dap")
    standardized_edges, gate_pre, split_pre, source_masked, target_masked = sigmoid_pieces(
        edge_entry, linear_mapping, latent_tensor
    )
    sigmoid_factor = jax.nn.sigmoid(gate_pre)
    tri_wide = triangle.astype(jnp.float32)
    unit_norm = truncated_numbers(edge_standardized(tri_wide, 0))
    values = jnp.einsum("crn,cz->rnz", unit_norm, final, preferred_element_type=jnp.float32)
    scaled = truncated_numbers(gradient * sigmoid_factor)
    final_sum = jnp.einsum("crn,rnz->cz", unit_norm, scaled, preferred_element_type=jnp.float32)
    grad_unit = jnp.einsum("rnz,cz->crn", scaled, final, preferred_element_type=jnp.float32)
    adjoint_sigmoid = truncated_numbers(gradient * values * sigmoid_factor * (1.0 - sigmoid_factor))
    grad_triangle = truncated_numbers(standardizer_adjoint(tri_wide, grad_unit, 0))
    (gradient_cols,) = to_channels(grad_triangle)
    left_back, right_back = contract_back_items(gradient_cols, kept[0], kept[1], outgoing)
    source_adjoint, target_adjoint = [
        values.astype(jnp.float32) for values in to_rows(left_back, right_back)
    ]
    logistic_primary = jax.nn.sigmoid(split_pre[:latent_tensor])
    logistic_tertiary = jax.nn.sigmoid(split_pre[2 * latent_tensor : 3 * latent_tensor])
    grad_split = truncated_numbers(
        jnp.concatenate(
            [
                source_adjoint
                * split_pre[latent_tensor : 2 * latent_tensor]
                * logistic_primary
                * (1.0 - logistic_primary),
                source_adjoint * logistic_primary,
                target_adjoint
                * split_pre[3 * latent_tensor :]
                * logistic_tertiary
                * (1.0 - logistic_tertiary),
                target_adjoint * logistic_tertiary,
            ],
            axis=0,
        )
    )
    proj_sum = jnp.concatenate(
        [
            jnp.einsum(
                "rnz,crn->zc", standardized_edges, grad_split, preferred_element_type=jnp.float32
            ),
            jnp.einsum(
                "rnz,rnc->zc",
                standardized_edges,
                adjoint_sigmoid,
                preferred_element_type=jnp.float32,
            ),
        ],
        axis=1,
    )
    grad_norm = jnp.einsum(
        "crn,zc->rnz",
        grad_split,
        linear_mapping[:, : 4 * latent_tensor],
        preferred_element_type=jnp.float32,
    )
    grad_norm = grad_norm + jnp.dot(
        adjoint_sigmoid,
        linear_mapping[:, 4 * latent_tensor :].T,
        preferred_element_type=jnp.float32,
    )
    grad_pair = gradient + standardizer_adjoint(edge_entry.astype(jnp.float32), grad_norm, 2)
    return (grad_pair, proj_sum, final_sum)


def shards(
    edge_embedding,
    alignment_embedding,
    tensor_flank_matrix,
    tensor_final_matrix,
    outward_sigmoid_matrix,
    outward_final_matrix,
    inward_sigmoid_matrix,
    inward_final_matrix,
    adjoint_seed,
):
    rows_here = edge_embedding.shape[0]
    residues = edge_embedding.shape[1]
    alignment_depth = alignment_embedding.shape[0]
    contraction_extent = tensor_flank_matrix.shape[1] // 2
    alignment_standardized = truncated_numbers(
        edge_standardized(alignment_embedding.astype(jnp.float32), 2)
    )
    alignment_mapped = jnp.dot(
        alignment_standardized, tensor_flank_matrix, preferred_element_type=jnp.float32
    )
    tensor_source_factor = truncated_numbers(alignment_mapped[..., :contraction_extent])
    tensor_target_factor = truncated_numbers(alignment_mapped[..., contraction_extent:])
    right_all = gathered(tensor_target_factor, 1).reshape(
        alignment_depth, residues, contraction_extent
    )
    tile_lines = 128 if residues % 128 == 0 else residues
    tile_number = residues // tile_lines
    outer_parts = []
    first_parts = []
    for block_index in range(tile_number):
        lower = block_index * tile_lines
        right_block = right_all[:, lower : lower + tile_lines]
        triangle_contraction = jnp.einsum(
            "sic,sjd->ijcd", tensor_source_factor, right_block, preferred_element_type=jnp.float32
        )
        outer_block = truncated_numbers(
            triangle_contraction.reshape(
                rows_here, tile_lines, contraction_extent * contraction_extent
            )
            / alignment_depth
        )
        update = jnp.dot(outer_block, tensor_final_matrix, preferred_element_type=jnp.float32)
        first_parts.append(
            truncated_numbers(
                edge_embedding[:, lower : lower + tile_lines].astype(jnp.float32) + update
            )
        )
        outer_parts.append(outer_block)
    outer_mean = jnp.concatenate(outer_parts, axis=1)
    pair_one = jnp.concatenate(first_parts, axis=1)
    pair_two, triangle_out, kept_out = triangle_forward(
        pair_one, outward_sigmoid_matrix, outward_final_matrix, True
    )
    edge_embedding_updated, triangle_in, kept_in = triangle_forward(
        pair_two, inward_sigmoid_matrix, inward_final_matrix, False
    )
    grad_two, inward_sigmoid_accrual, inward_final_accrual = triangle_back(
        pair_two,
        inward_sigmoid_matrix,
        inward_final_matrix,
        False,
        triangle_in,
        kept_in,
        adjoint_seed.astype(jnp.float32),
    )
    grad_one, outward_sigmoid_accrual, outward_final_accrual = triangle_back(
        pair_one, outward_sigmoid_matrix, outward_final_matrix, True, triangle_out, kept_out, grad_two
    )
    edge_embedding_adjoint = truncated_numbers(grad_one)
    tensor_final_accrual = jnp.einsum(
        "rnk,rnz->kz", outer_mean, edge_embedding_adjoint, preferred_element_type=jnp.float32
    )
    source_adjoint = jnp.zeros((alignment_depth, rows_here, contraction_extent), jnp.float32)
    outer_grads = []
    for block_index in range(tile_number):
        lower = block_index * tile_lines
        right_block = right_all[:, lower : lower + tile_lines]
        adjoint_tensor_mean = truncated_numbers(
            jnp.dot(
                edge_embedding_adjoint[:, lower : lower + tile_lines],
                tensor_final_matrix.T,
                preferred_element_type=jnp.float32,
            )
        )
        adjoint_tensor_mean = adjoint_tensor_mean.reshape(
            rows_here, tile_lines, contraction_extent, contraction_extent
        )
        source_adjoint = (
            source_adjoint
            + jnp.einsum(
                "mopz,loz->lmp",
                adjoint_tensor_mean,
                right_block,
                preferred_element_type=jnp.float32,
            )
            / alignment_depth
        )
        outer_grads.append(adjoint_tensor_mean)
    pair_columns = lax.all_to_all(
        edge_embedding_adjoint, "dap", split_axis=1, concat_axis=0, tiled=True
    )
    left_all = gathered(tensor_source_factor, 1).reshape(
        alignment_depth, residues, contraction_extent
    )
    target_adjoint = jnp.zeros((alignment_depth, rows_here, contraction_extent), jnp.float32)
    for block_index in range(tile_number):
        lower = block_index * tile_lines
        column_grad = truncated_numbers(
            jnp.dot(
                pair_columns[lower : lower + tile_lines],
                tensor_final_matrix.T,
                preferred_element_type=jnp.float32,
            )
        )
        column_grad = column_grad.reshape(
            tile_lines, rows_here, contraction_extent, contraction_extent
        )
        target_adjoint = (
            target_adjoint
            + jnp.einsum(
                "gxqp,vgq->vxp",
                column_grad,
                left_all[:, lower : lower + tile_lines],
                preferred_element_type=jnp.float32,
            )
            / alignment_depth
        )
    alignment_mapped_adjoint = truncated_numbers(
        jnp.concatenate([source_adjoint, target_adjoint], axis=2)
    )
    tensor_flank_accrual = jnp.einsum(
        "ajo,ajm->om",
        alignment_standardized,
        alignment_mapped_adjoint,
        preferred_element_type=jnp.float32,
    )
    alignment_standard_adjoint = jnp.dot(
        alignment_mapped_adjoint, tensor_flank_matrix.T, preferred_element_type=jnp.float32
    )
    alignment_adjoint = truncated_numbers(
        standardizer_adjoint(alignment_embedding.astype(jnp.float32), alignment_standard_adjoint, 2)
    )
    totals = totalled(
        (
            tensor_flank_accrual,
            tensor_final_accrual,
            outward_sigmoid_accrual,
            outward_final_accrual,
            inward_sigmoid_accrual,
            inward_final_accrual,
        )
    )
    return (
        edge_embedding_updated,
        edge_embedding_adjoint,
        alignment_adjoint,
        totals[0] / residues,
        totals[1] / residues,
        totals[2] / residues,
        totals[3] / residues,
        totals[4] / residues,
        totals[5] / residues,
    )


F32 = jnp.float32
BF16 = jnp.bfloat16
LANES = 128
SUB = 8


def nn(a, b):
    return lax.dot_general(a, b, (((1,), (0,)), ((), ())), preferred_element_type=F32)


def nt(a, b):
    return lax.dot_general(a, b, (((1,), (1,)), ((), ())), preferred_element_type=F32)


def tn(a, b):
    return lax.dot_general(a, b, (((0,), (0,)), ((), ())), preferred_element_type=F32)


def launch(body, outs, args, scratch=(), name=None, flops=2e8, raw=False):
    vmem = pl.BlockSpec(memory_space=pltpu.VMEM)
    held = pl.BlockSpec(memory_space=pltpu.HBM) if raw else vmem
    if raw:
        args = [pltpu.with_memory_space_constraint(a, pltpu.HBM) for a in args]
    moved = sum(a.size * a.dtype.itemsize for a in args) + sum(
        o.size * o.dtype.itemsize for o in outs
    )
    return pl.pallas_call(
        body,
        out_shape=outs,
        in_specs=[held] * len(args),
        out_specs=[vmem] * len(outs),
        scratch_shapes=list(scratch),
        name=name,
        cost_estimate=pl.CostEstimate(
            flops=int(flops), bytes_accessed=int(moved), transcendentals=0
        ),
        compiler_params=pltpu.CompilerParams(vmem_limit_bytes=24 * 1024 * 1024),
    )(*args)


def moments(x, axis):
    average = jnp.mean(x, axis=axis, keepdims=True)
    centred = x - average
    factor = lax.rsqrt(jnp.mean(centred * centred, axis=axis, keepdims=True) + EPSILON)
    return centred * factor, factor


def moments_adjoint(hatted, factor, gradient, axis):
    return factor * (
        gradient
        - jnp.mean(gradient, axis=axis, keepdims=True)
        - hatted * jnp.mean(gradient * hatted, axis=axis, keepdims=True)
    )


def tall(x):
    if x.shape[0] == LANES:
        return x
    return jnp.concatenate([x, jnp.zeros((LANES - x.shape[0], x.shape[1]), x.dtype)], axis=0)


def dealt(x, groups):
    return x.reshape((groups, x.shape[0] // groups) + x.shape[1:])


def gated_pair(projected, width):
    left = jax.nn.sigmoid(projected[:width]) * projected[width : 2 * width]
    right = jax.nn.sigmoid(projected[2 * width : 3 * width]) * projected[3 * width : 4 * width]
    return left, right


def lanes_of(x):
    return lax.broadcasted_iota(jnp.int32, x.shape, x.ndim - 1)


def shifted(x, amount):
    amount = amount % LANES
    return x if amount == 0 else pltpu.roll(x, amount, x.ndim - 1)


def split_rows(tiles, rows, residues):
    out = []
    lane = lanes_of(tiles[0])
    for row in range(rows):
        tile, offset = divmod(row * residues, LANES)
        piece = shifted(tiles[tile], -offset)
        if offset + residues > LANES:
            piece = jnp.where(lane < LANES - offset, piece, shifted(tiles[tile + 1], -offset))
        out.append(jnp.where(lane < residues, piece, 0.0))
    return out


def join_rows(values, residues, count):
    out = [None] * count
    lane = lanes_of(values[0])
    for row, value in enumerate(values):
        tile, offset = divmod(row * residues, LANES)
        moved = shifted(value, offset)
        out[tile] = moved if out[tile] is None else jnp.where(lane >= offset, moved, out[tile])
        if offset + residues > LANES:
            out[tile + 1] = jnp.where(lane < offset + residues - LANES, moved, 0.0)
    return out


class Layout:
    def __init__(self, rows, residues, share):
        self.rows, self.residues, self.share = rows, residues, share
        self.cells = rows * residues
        self.tiles = -(-self.cells // LANES)
        self.spots = self.tiles * LANES
        rest = self.cells % LANES
        self.paired = 0 < rest <= LANES // 2
        self.single = self.tiles * share
        self.double = self.tiles * 2 * share - (share if self.paired else 0)

    def shared(self, tile):
        return self.paired and tile == self.tiles - 1

    def lanes(self, tile):
        return slice(tile * LANES, (tile + 1) * LANES)

    def filled(self, tile):
        return min(LANES, self.cells - tile * LANES)

    def pack(self, out_ref, tile, left, right):
        start = tile * 2 * self.share
        if self.shared(tile):
            both = jnp.where(lanes_of(left) < LANES // 2, left, shifted(right, LANES // 2))
        else:
            both = jnp.concatenate([left, right], axis=1)
        out_ref[:, start : start + both.shape[1], :] = both.astype(BF16)

    def unpack(self, both_ref, tile):
        start = tile * 2 * self.share
        left = both_ref[:, start : start + self.share, :].astype(F32)
        if self.shared(tile):
            low = lanes_of(left) < LANES // 2
            right = jnp.where(low, shifted(left, LANES // 2), 0.0)
            return jnp.where(low, left, 0.0), right
        start += self.share
        return left, both_ref[:, start : start + self.share, :].astype(F32)

    def spread_pairs(self, both_ref, wide_ref):
        tiles = [
            jnp.concatenate(self.unpack(both_ref, tile), axis=1) for tile in range(self.tiles)
        ]
        self.spread(tiles, wide_ref)

    def spread_singles(self, grad_ref, wide_ref):
        tiles = [
            grad_ref[:, tile * self.share : (tile + 1) * self.share, :].astype(F32)
            for tile in range(self.tiles)
        ]
        self.spread(tiles, wide_ref)

    def spread(self, tiles, wide_ref):
        wide = tiles[0].shape[1]
        for row, value in enumerate(split_rows(tiles, self.rows, self.residues)):
            for group in range(value.shape[0]):
                at = (group * self.rows + row) * wide
                wide_ref[at : at + wide, :] = value[group]

    def collect(self, result_ref, groups):
        wide = result_ref.shape[0] // (groups * self.rows)
        whole = result_ref[...].reshape(groups, self.rows * wide, LANES)
        values = [whole[:, row * wide : (row + 1) * wide, :] for row in range(self.rows)]
        return join_rows(values, self.residues, self.tiles)


def turned(to_ref, from_ref):
    for tile in range(from_ref.shape[1] // LANES):
        lanes = slice(tile * LANES, (tile + 1) * LANES)
        to_ref[lanes, :] = from_ref[:, lanes].astype(F32).T.astype(BF16)


def msa_kernel(sizes, *refs):
    rows, depth, hidden, groups = sizes
    sources, refs = refs[:7], refs[7:]
    (
        send_ref,
        normal_ref,
        left_ref,
        sorted_ref,
        sorted_t_ref,
        gates_out_t_ref,
        gates_in_t_ref,
        final_out_t_ref,
        final_in_t_ref,
    ) = refs[:9]
    held, wide_ref, semaphores = refs[9:16], refs[16], refs[17]
    copies = [
        pltpu.make_async_copy(source, target, semaphores.at[at])
        for at, (source, target) in enumerate(zip(sources, held))
    ]
    for copy in copies:
        copy.start()
    msa_ref, flank_t_ref, final_ref, gates_out_ref, gates_in_ref, final_out_ref, final_in_ref = held
    copies[0].wait()
    copies[1].wait()
    for row in range(rows):
        hatted, _ = moments(msa_ref[row].astype(F32), 1)
        normal = hatted.astype(BF16)
        normal_ref[row] = normal
        twice = jnp.concatenate([normal, normal], axis=0)
        mapped = nt(flank_t_ref[...], twice)
        low = lax.broadcasted_iota(jnp.int32, (hidden, LANES), 1) < depth
        left = mapped[:hidden]
        left_ref[row * hidden : (row + 1) * hidden] = jnp.where(low, left, 0.0).astype(BF16)
        left_ref[(rows + row) * hidden : (rows + row + 1) * hidden] = jnp.where(
            low, 0.0, left
        ).astype(BF16)
        half = hidden // 2
        right = jnp.where(
            low[:half], mapped[hidden : hidden + half], mapped[hidden + half :]
        ).astype(BF16)
        for group in range(groups):
            send_ref[group, row * half : (row + 1) * half, :] = right
    for copy in copies[2:]:
        copy.wait()
    wide_ref[...] = final_ref[...].astype(F32)
    for d in range(hidden):
        sorted_ref[d * hidden : (d + 1) * hidden, :] = wide_ref[
            pl.ds(d, hidden, stride=hidden), :
        ].astype(BF16)
    for tile in range(hidden * hidden // LANES):
        at = slice(tile * LANES, (tile + 1) * LANES)
        sorted_t_ref[:, at] = sorted_ref[at, :].astype(F32).T.astype(BF16)
    turned(gates_out_t_ref, gates_out_ref)
    turned(gates_in_t_ref, gates_in_ref)
    turned(final_out_t_ref, final_out_ref)
    turned(final_in_t_ref, final_in_ref)


def outer_kernel(
    sizes,
    right_ref,
    left_ref,
    edge_ref,
    final_t_ref,
    gates_t_ref,
    send_ref,
    spread_ref,
    outer_ref,
    pair_ref,
    wide_ref,
):
    layout, depth, hidden, groups, width = sizes
    rows, residues = layout.rows, layout.residues
    half = hidden // 2
    wide_ref[...] = right_ref[...].reshape(wide_ref.shape).astype(F32)
    for d in range(half):
        picked = wide_ref[pl.ds(d, residues, stride=half), :]
        spread_ref[d * LANES : (d + 1) * LANES, :] = tall(picked).astype(BF16)
    for d in range(0, half, 2):
        block = nt(left_ref[...], spread_ref[d * LANES : (d + 2) * LANES, :]) / depth
        for e in range(2):
            for h in range(2):
                for row in range(rows):
                    at = (h * rows + row) * hidden
                    to = (h * half + d + e) * hidden
                    outer_ref[to : to + hidden, row * LANES : (row + 1) * LANES] = block[
                        at : at + hidden, e * LANES : (e + 1) * LANES
                    ].astype(BF16)
    update = nn(final_t_ref[...], outer_ref[...])
    update = join_rows(
        [update[:, row * LANES : (row + 1) * LANES] for row in range(rows)], residues, layout.tiles
    )
    for tile in range(layout.tiles):
        lanes = layout.lanes(tile)
        at = tile * LANES
        entry = tall(edge_ref[at : at + layout.filled(tile), :].astype(F32)).T
        pair = (entry + update[tile]).astype(BF16)
        pair_ref[:, lanes] = pair
        hatted, _ = moments(pair.astype(F32), 0)
        projected = nn(gates_t_ref[: 4 * width, :], hatted.astype(BF16))
        left, right = gated_pair(projected, width)
        layout.pack(send_ref, tile, dealt(left, groups), dealt(right, groups))


def triangle_kernel(sizes, outgoing, both_ref, send_ref, wide_ref, result_ref):
    layout, groups = sizes
    residues, share = layout.residues, layout.share
    layout.spread_pairs(both_ref, wide_ref)
    for c in range(share):
        left = wide_ref[pl.ds(c, residues, stride=2 * share), :].astype(BF16)
        right = wide_ref[pl.ds(share + c, residues, stride=2 * share), :].astype(BF16)
        if outgoing:
            product = nt(left, tall(right))
        else:
            product = tn(left, right)[:residues]
        result_ref[pl.ds(c, residues, stride=share), :] = product
    for tile, value in enumerate(layout.collect(result_ref, groups)):
        send_ref[:, tile * share : (tile + 1) * share, :] = value.astype(BF16)


def triangle_adjoint_kernel(
    sizes, outgoing, both_ref, grad_ref, send_ref, wide_ref, tri_ref, result_ref
):
    layout, groups, riders = sizes
    residues, share = layout.residues, layout.share
    layout.spread_pairs(both_ref, wide_ref)
    layout.spread_singles(grad_ref, tri_ref)
    for c in range(share):
        left = wide_ref[pl.ds(c, residues, stride=2 * share), :].astype(BF16)
        right = wide_ref[pl.ds(share + c, residues, stride=2 * share), :].astype(BF16)
        grad = tri_ref[pl.ds(c, residues, stride=share), :].astype(BF16)
        if outgoing:
            grad_left = nn(grad, tall(right))
            grad_right = tn(grad, left)[:residues]
        else:
            grad_left = nt(right, tall(grad))
            grad_right = nn(left, tall(grad))
        result_ref[pl.ds(c, residues, stride=2 * share), :] = grad_left
        result_ref[pl.ds(share + c, residues, stride=2 * share), :] = grad_right
    for tile, value in enumerate(layout.collect(result_ref, groups)):
        layout.pack(send_ref, tile, value[:, :share, :], value[:, share:, :])
    if riders:
        summed = jnp.sum(grad_ref[:, layout.single :, :].astype(F32), axis=0).astype(BF16)
        for group in range(groups):
            send_ref[group, layout.double :, :] = summed


def tri_tile(layout, tri_ref, tile, width):
    share = layout.share
    return tri_ref[:, tile * share : (tile + 1) * share, :].astype(F32).reshape(width, LANES)


def middle_kernel(
    sizes,
    tri_ref,
    pair_ref,
    gates_t_ref,
    final_t_ref,
    next_gates_t_ref,
    send_ref,
    next_ref,
):
    layout, groups, width = sizes
    for tile in range(layout.tiles):
        lanes = layout.lanes(tile)
        tri = tri_tile(layout, tri_ref, tile, width)
        unit, _ = moments(tri, 0)
        values = nn(final_t_ref[...], unit.astype(BF16))
        pair = pair_ref[:, lanes].astype(F32)
        hatted, _ = moments(pair, 0)
        gate = jax.nn.sigmoid(nn(gates_t_ref[4 * width :, :], hatted.astype(BF16)))
        following = (pair + gate * values).astype(BF16)
        next_ref[:, lanes] = following
        hatted, _ = moments(following.astype(F32), 0)
        projected = nn(next_gates_t_ref[: 4 * width, :], hatted.astype(BF16))
        left, right = gated_pair(projected, width)
        layout.pack(send_ref, tile, dealt(left, groups), dealt(right, groups))


def tri_adjoint_row(tri, pair, gradient, gates_t_ref, final_ref, final_t_ref, width):
    hatted_tri, factor = moments(tri, 0)
    unit = hatted_tri.astype(BF16)
    values = nn(final_t_ref[...], unit)
    hatted, _ = moments(pair, 0)
    gate = jax.nn.sigmoid(nn(gates_t_ref[4 * width :, :], hatted.astype(BF16)))
    scaled = (gradient * gate).astype(BF16)
    grad_unit = nn(final_ref[...], scaled)
    grad_tri = moments_adjoint(hatted_tri, factor, grad_unit, 0)
    grad_gate = (gradient * values * gate * (1.0 - gate)).astype(BF16)
    return unit, scaled, values, gate, grad_tri, grad_gate


def turn_kernel(
    sizes,
    tri_ref,
    pair_ref,
    seed_ref,
    gates_t_ref,
    final_ref,
    final_t_ref,
    send_ref,
    out_ref,
    seed_t_ref,
    grad_gate_ref,
    final_sum_ref,
    grads_ref,
    unit_ref,
    scaled_ref,
):
    layout, groups, width = sizes
    share = layout.share
    for tile in range(layout.tiles):
        lanes = layout.lanes(tile)
        at = tile * LANES
        filled = layout.filled(tile)
        tri = tri_tile(layout, tri_ref, tile, width)
        pair = pair_ref[:, lanes].astype(F32)
        gradient = tall(seed_ref[at : at + filled, :].astype(F32)).T
        seed_t_ref[:, lanes] = gradient.astype(BF16)
        unit, scaled, values, gate, grad_tri, grad_gate = tri_adjoint_row(
            tri, pair, gradient, gates_t_ref, final_ref, final_t_ref, width
        )
        unit_ref[:, lanes] = unit
        scaled_ref[:, lanes] = scaled
        grad_gate_ref[:, lanes] = grad_gate
        grads_ref[:, tile * share : (tile + 1) * share, :] = dealt(grad_tri, groups)
        out_ref[at : at + filled, :] = (pair + gate * values).T[:filled].astype(BF16)
    send_ref[...] = grads_ref[...].astype(BF16)
    final_sum_ref[...] = nt(unit_ref[...], scaled_ref[...])


def proj_adjoint_row(
    layout, tile, both_ref, pair, grad_gate, gates_t_ref, gates_ref, normal_ref, proj_ref, width
):
    lanes = layout.lanes(tile)
    grad_left, grad_right = layout.unpack(both_ref, tile)
    grad_left = grad_left.reshape(width, LANES)
    grad_right = grad_right.reshape(width, LANES)
    hatted, factor = moments(pair, 0)
    normal = hatted.astype(BF16)
    normal_ref[:, lanes] = normal
    projected = nn(gates_t_ref[: 4 * width, :], normal)
    first = jax.nn.sigmoid(projected[:width])
    third = jax.nn.sigmoid(projected[2 * width : 3 * width])
    left_part = grad_left * first
    right_part = grad_right * third
    proj_ref[:width, lanes] = (
        left_part * projected[width : 2 * width] * (1.0 - first)
    ).astype(BF16)
    proj_ref[width : 2 * width, lanes] = left_part.astype(BF16)
    proj_ref[2 * width : 3 * width, lanes] = (
        right_part * projected[3 * width :] * (1.0 - third)
    ).astype(BF16)
    proj_ref[3 * width : 4 * width, lanes] = right_part.astype(BF16)
    proj_ref[4 * width :, lanes] = grad_gate
    grad_normal = nn(gates_ref[...], proj_ref[:, lanes])
    return moments_adjoint(hatted, factor, grad_normal, 0)


def deal_rows(out_ref, start, total, groups):
    for tile in range(total.shape[1] // LANES):
        block = dealt(total[:, tile * LANES : (tile + 1) * LANES], groups)
        out_ref[:, start : start + block.shape[1], :] = block
        start += block.shape[1]
    return start


def between_kernel(
    sizes,
    both_ref,
    pair_in_ref,
    seed_ref,
    grad_gate_in_ref,
    gates_in_t_ref,
    gates_in_ref,
    final_in_sum_ref,
    tri_ref,
    pair_out_ref,
    gates_out_t_ref,
    final_out_ref,
    final_out_t_ref,
    send_ref,
    grad_ref,
    grad_gate_ref,
    grads_ref,
    normal_ref,
    proj_ref,
    unit_ref,
    scaled_ref,
):
    layout, groups, width = sizes
    share = layout.share
    for tile in range(layout.tiles):
        lanes = layout.lanes(tile)
        pair = pair_in_ref[:, lanes].astype(F32)
        gradient = seed_ref[:, lanes].astype(F32) + proj_adjoint_row(
            layout,
            tile,
            both_ref,
            pair,
            grad_gate_in_ref[:, lanes],
            gates_in_t_ref,
            gates_in_ref,
            normal_ref,
            proj_ref,
            width,
        )
        grad_ref[:, lanes] = gradient
        tri = tri_tile(layout, tri_ref, tile, width)
        unit, scaled, _, _, grad_tri, grad_gate = tri_adjoint_row(
            tri,
            pair_out_ref[:, lanes].astype(F32),
            gradient,
            gates_out_t_ref,
            final_out_ref,
            final_out_t_ref,
            width,
        )
        unit_ref[:, lanes] = unit
        scaled_ref[:, lanes] = scaled
        grad_gate_ref[:, lanes] = grad_gate
        grads_ref[:, tile * share : (tile + 1) * share, :] = dealt(grad_tri, groups)
    place = layout.single
    place = deal_rows(grads_ref, place, nt(normal_ref[...], proj_ref[...]), groups)
    place = deal_rows(grads_ref, place, final_in_sum_ref[...], groups)
    deal_rows(grads_ref, place, nt(unit_ref[...], scaled_ref[...]), groups)
    send_ref[...] = grads_ref[...].astype(BF16)


def gathered_rows(rest, start, tiles, width):
    out = []
    share = width // rest.shape[0]
    for tile in range(tiles):
        out.append(rest[:, start + tile * share : start + (tile + 1) * share, :].reshape(width, LANES))
    return out, start + tiles * share


def close_kernel(
    sizes,
    both_ref,
    pair_ref,
    grad_ref,
    grad_gate_ref,
    gates_t_ref,
    gates_ref,
    outer_ref,
    final_ref,
    spread_ref,
    left_ref,
    msa_normal_ref,
    send_ref,
    adjoint_ref,
    left_grad_ref,
    grads_ref,
    normal_ref,
    proj_ref,
    adjoint_t_ref,
    outer_grad_ref,
    right_grad_ref,
):
    layout, depth, hidden, groups, width = sizes
    rows, residues = layout.rows, layout.residues
    half = hidden // 2
    adjoints = []
    for tile in range(layout.tiles):
        lanes = layout.lanes(tile)
        gradient = grad_ref[:, lanes] + proj_adjoint_row(
            layout,
            tile,
            both_ref,
            pair_ref[:, lanes].astype(F32),
            grad_gate_ref[:, lanes],
            gates_t_ref,
            gates_ref,
            normal_ref,
            proj_ref,
            width,
        )
        adjoint = gradient.astype(BF16).astype(F32)
        adjoints.append(adjoint)
        at = tile * LANES
        filled = layout.filled(tile)
        adjoint_ref[at : at + filled, :] = adjoint.T[:filled].astype(BF16)
    for row, value in enumerate(split_rows(adjoints, rows, residues)):
        adjoint = value.astype(BF16)
        adjoint_t_ref[:, row * LANES : (row + 1) * LANES] = adjoint
        spread_grad = nn(final_ref[...], adjoint).astype(BF16)
        for h in range(2):
            for d in range(half):
                at = (h * half + d) * hidden
                to = (h * rows + row) * hidden
                outer_grad_ref[to : to + hidden, d * LANES : (d + 1) * LANES] = spread_grad[
                    at : at + hidden
                ]
    for d in range(half):
        piece = tn(outer_grad_ref[:, d * LANES : (d + 1) * LANES], left_ref[...]) / depth
        right_grad_ref[pl.ds(d, residues, stride=half), :] = piece[:residues]
    own = rows * half
    grads_ref[:, :own, :] = right_grad_ref[...].reshape(groups, own, LANES)
    place = deal_rows(grads_ref, own, nt(normal_ref[...], proj_ref[...]), groups)
    outer_sum = nt(outer_ref[...], adjoint_t_ref[...])
    place = deal_rows(grads_ref, place, outer_sum, groups)
    stacked = nn(outer_grad_ref[...], spread_ref[...]) / depth
    count = rows * hidden
    lane = lax.broadcasted_iota(jnp.int32, (count, LANES), 1)
    left_grad = jnp.where(
        lane < depth, stacked[:count] + pltpu.roll(stacked[count:], LANES - depth, 1), 0.0
    ).astype(BF16)
    left_grad_ref[...] = left_grad
    flank = jnp.zeros((hidden, msa_normal_ref.shape[2]), F32)
    for row in range(rows):
        flank = flank + nn(
            left_grad[row * hidden : (row + 1) * hidden, :depth], msa_normal_ref[row]
        )
    for tile in range(flank.shape[1] // LANES):
        part = flank[:, tile * LANES : (tile + 1) * LANES].reshape(hidden // SUB, SUB, LANES)
        spare = tile * (hidden // SUB)
        grads_ref[spare : spare + hidden // SUB, place : place + SUB, :] = part
    used = (flank.shape[1] // LANES) * (hidden // SUB)
    grads_ref[used:, place : place + SUB, :] = jnp.zeros((groups - used, SUB, LANES), F32)
    send_ref[...] = grads_ref[...].astype(BF16)


def msa_adjoint_kernel(
    sizes,
    parts_ref,
    left_grad_ref,
    msa_ref,
    msa_normal_ref,
    flank_t_ref,
    send_ref,
    adjoint_ref,
):
    rows, depth, hidden, groups = sizes
    half = hidden // 2
    own = rows * half
    summed = jnp.sum(parts_ref[...].astype(F32), axis=0).astype(BF16)
    right = summed[:own].astype(F32)
    flank = jnp.zeros((hidden, msa_normal_ref.shape[2]), F32)
    for row in range(rows):
        part = right[row * half : (row + 1) * half]
        right_grad = jnp.concatenate([part, pltpu.roll(part, LANES - depth, 1)], axis=0)[
            :, :depth
        ].astype(BF16)
        left_grad = left_grad_ref[row * hidden : (row + 1) * hidden, :depth]
        flank = flank + nn(right_grad, msa_normal_ref[row])
        grad = jnp.concatenate([left_grad, right_grad], axis=0)
        gradient = tn(grad, flank_t_ref[...])
        hatted, factor = moments(msa_ref[row].astype(F32), 1)
        adjoint_ref[row] = moments_adjoint(hatted, factor, gradient, 1).astype(BF16)
    rest = summed[own:]
    flank = flank.astype(BF16)
    for group in range(groups):
        send_ref[group, : rest.shape[0], :] = rest
        for tile in range(flank.shape[1] // LANES):
            at = rest.shape[0] + tile * hidden
            send_ref[group, at : at + hidden, :] = flank[:, tile * LANES : (tile + 1) * LANES]


def totals_kernel(
    sizes,
    parts_ref,
    both_ref,
    updated_ref,
    adjoint_ref,
    proj_ref,
    final_ref,
    flank_ref,
    proj_in_ref,
    final_in_ref,
    final_out_ref,
    updated_out_ref,
    adjoint_out_ref,
    wide_ref,
):
    layout, hidden, groups, width = sizes
    residues = layout.residues
    updated_out_ref[...] = updated_ref[...]
    adjoint_out_ref[...] = adjoint_ref[...]
    rest = both_ref[:, layout.double :, :].astype(F32)
    tiles, place = gathered_rows(rest, 0, proj_in_ref.shape[1] // LANES, width)
    for tile, value in enumerate(tiles):
        proj_in_ref[:, tile * LANES : (tile + 1) * LANES] = value / residues
    for target_ref in (final_in_ref, final_out_ref):
        tiles, place = gathered_rows(rest, place, 1, width)
        target_ref[...] = tiles[0] / residues
    parts = parts_ref[...].astype(F32)
    tiles, place = gathered_rows(parts, 0, proj_ref.shape[1] // LANES, width)
    for tile, value in enumerate(tiles):
        proj_ref[:, tile * LANES : (tile + 1) * LANES] = value / residues
    share = wide_ref.shape[0] // groups
    wide_ref[...] = parts[:, place : place + share, :].reshape(wide_ref.shape) / residues
    for c in range(hidden):
        final_ref[c * hidden : (c + 1) * hidden, :] = wide_ref[pl.ds(c, hidden, stride=hidden), :]
    place += share
    blocks = hidden // SUB
    for tile in range(flank_ref.shape[1] // LANES):
        lanes = slice(tile * LANES, (tile + 1) * LANES)
        left = parts[tile * blocks : (tile + 1) * blocks, place : place + SUB, :]
        flank_ref[:hidden, lanes] = left.reshape(hidden, LANES) / residues
        at = place + SUB + tile * hidden
        flank_ref[hidden:, lanes] = jnp.sum(parts[:, at : at + hidden, :], axis=0) / residues


def kernel_shards(
    edge_embedding,
    alignment_embedding,
    tensor_flank_matrix,
    tensor_final_matrix,
    outward_sigmoid_matrix,
    outward_final_matrix,
    inward_sigmoid_matrix,
    inward_final_matrix,
    adjoint_seed,
):
    groups = lax.axis_size("dap")
    rows, residues, width = edge_embedding.shape
    depth, _, features = alignment_embedding.shape
    hidden = tensor_flank_matrix.shape[1] // 2
    half = hidden // 2
    share = width // groups
    layout = Layout(rows, residues, share)
    spots = layout.spots
    square = hidden * hidden

    def shape(*dims, dtype=BF16):
        return jax.ShapeDtypeStruct(dims, dtype)

    msa = jnp.swapaxes(alignment_embedding, 0, 1)
    flank_t = tensor_flank_matrix.T
    (
        send,
        msa_normal,
        left,
        final_sorted,
        final_sorted_t,
        gates_out_t,
        gates_in_t,
        final_out_t,
        final_in_t,
    ) = launch(
        partial(msa_kernel, (rows, depth, hidden, groups)),
        [
            shape(groups, rows * half, LANES),
            shape(rows, depth, features),
            shape(2 * rows * hidden, LANES),
            shape(square, width),
            shape(width, square),
            shape(5 * width, width),
            shape(5 * width, width),
            shape(width, width),
            shape(width, width),
        ],
        (
            msa,
            flank_t,
            tensor_final_matrix,
            outward_sigmoid_matrix,
            inward_sigmoid_matrix,
            outward_final_matrix,
            inward_final_matrix,
        ),
        [
            pltpu.VMEM((rows, depth, features), BF16),
            pltpu.VMEM((2 * hidden, features), BF16),
            pltpu.VMEM((square, width), BF16),
            pltpu.VMEM((width, 5 * width), BF16),
            pltpu.VMEM((width, 5 * width), BF16),
            pltpu.VMEM((width, width), BF16),
            pltpu.VMEM((width, width), BF16),
            pltpu.VMEM((square, width), F32),
            pltpu.SemaphoreType.DMA((7,)),
        ],
        name="msa",
        raw=True,
    )
    right = exchanged(send)

    send, spread, outer, pair_one = launch(
        partial(outer_kernel, (layout, depth, hidden, groups, width)),
        [
            shape(groups, layout.double, LANES),
            shape(half * LANES, LANES),
            shape(square, rows * LANES),
            shape(width, spots),
        ],
        (right, left, edge_embedding.reshape(-1, width), final_sorted_t, gates_out_t),
        [pltpu.VMEM((residues * half, LANES), F32)],
        name="outer",
    )

    def triangle(both, outgoing):
        return launch(
            partial(triangle_kernel, (layout, groups), outgoing),
            [shape(groups, layout.single, LANES)],
            (both,),
            [
                pltpu.VMEM((residues * 2 * share, LANES), F32),
                pltpu.VMEM((residues * share, LANES), F32),
            ],
            name="triangle_out" if outgoing else "triangle_in",
        )[0]

    def triangle_adjoint(both, grads, outgoing):
        riders = grads.shape[1] - layout.single
        return launch(
            partial(triangle_adjoint_kernel, (layout, groups, riders), outgoing),
            [shape(groups, layout.double + riders, LANES)],
            (both, grads),
            [
                pltpu.VMEM((residues * 2 * share, LANES), F32),
                pltpu.VMEM((residues * share, LANES), F32),
                pltpu.VMEM((residues * 2 * share, LANES), F32),
            ],
            name="adjoint_out" if outgoing else "adjoint_in",
        )[0]

    both_out = exchanged(send)
    tri_out = exchanged(triangle(both_out, True))
    send, pair_two = launch(
        partial(middle_kernel, (layout, groups, width)),
        [shape(groups, layout.double, LANES), shape(width, spots)],
        (tri_out, pair_one, gates_out_t, final_out_t, gates_in_t),
        name="middle",
    )
    both_in = exchanged(send)
    tri_in = exchanged(triangle(both_in, False))
    send, updated, seed_t, grad_gate_in, final_in_sum = launch(
        partial(turn_kernel, (layout, groups, width)),
        [
            shape(groups, layout.single, LANES),
            shape(rows * residues, width),
            shape(width, spots),
            shape(width, spots),
            shape(width, width, dtype=F32),
        ],
        (tri_in, pair_two, adjoint_seed.reshape(-1, width), gates_in_t, inward_final_matrix, final_in_t),
        [
            pltpu.VMEM((groups, layout.single, LANES), F32),
            pltpu.VMEM((width, spots), BF16),
            pltpu.VMEM((width, spots), BF16),
        ],
        name="turn",
    )
    grads = exchanged(triangle_adjoint(both_in, exchanged(send), False))
    riders = share * (gates_in_t.shape[0] // LANES + 2)
    send, grad_two, grad_gate_out = launch(
        partial(between_kernel, (layout, groups, width)),
        [
            shape(groups, layout.single + riders, LANES),
            shape(width, spots, dtype=F32),
            shape(width, spots),
        ],
        (
            grads,
            pair_two,
            seed_t,
            grad_gate_in,
            gates_in_t,
            inward_sigmoid_matrix,
            final_in_sum,
            tri_out,
            pair_one,
            gates_out_t,
            outward_final_matrix,
            final_out_t,
        ),
        [
            pltpu.VMEM((groups, layout.single + riders, LANES), F32),
            pltpu.VMEM((width, spots), BF16),
            pltpu.VMEM((5 * width, spots), BF16),
            pltpu.VMEM((width, spots), BF16),
            pltpu.VMEM((width, spots), BF16),
        ],
        name="between",
    )
    grads = exchanged(triangle_adjoint(both_out, exchanged(send), True))
    count = rows * half + share * 5 + square // groups + SUB
    send, edge_adjoint, left_grad = launch(
        partial(close_kernel, (layout, depth, hidden, groups, width)),
        [
            shape(groups, count, LANES),
            shape(rows * residues, width),
            shape(rows * hidden, LANES),
        ],
        (
            grads,
            pair_one,
            grad_two,
            grad_gate_out,
            gates_out_t,
            outward_sigmoid_matrix,
            outer,
            final_sorted,
            spread,
            left,
            msa_normal,
        ),
        [
            pltpu.VMEM((groups, count, LANES), F32),
            pltpu.VMEM((width, spots), BF16),
            pltpu.VMEM((5 * width, spots), BF16),
            pltpu.VMEM((width, rows * LANES), BF16),
            pltpu.VMEM((2 * rows * hidden, half * LANES), BF16),
            pltpu.VMEM((residues * half, LANES), F32),
        ],
        name="close",
    )
    rest = count - rows * half
    send, msa_adjoint = launch(
        partial(msa_adjoint_kernel, (rows, depth, hidden, groups)),
        [
            shape(groups, rest + hidden * features // LANES, LANES),
            shape(rows, depth, features),
        ],
        (exchanged(send), left_grad, msa, msa_normal, flank_t),
        name="msa_adjoint",
    )
    proj_out, outer_final, outer_proj_t, proj_in, final_in, final_out, updated, edge_adjoint = launch(
        partial(totals_kernel, (layout, hidden, groups, width)),
        [
            shape(width, 5 * width, dtype=F32),
            shape(square, width, dtype=F32),
            shape(2 * hidden, features, dtype=F32),
            shape(width, 5 * width, dtype=F32),
            shape(width, width, dtype=F32),
            shape(width, width, dtype=F32),
            shape(rows * residues, width),
            shape(rows * residues, width),
        ],
        (exchanged(send), grads, updated, edge_adjoint),
        [pltpu.VMEM((square, width), F32)],
        name="totals",
    )
    return (
        updated.reshape(edge_embedding.shape),
        edge_adjoint.reshape(edge_embedding.shape),
        jnp.swapaxes(msa_adjoint, 0, 1),
        outer_proj_t.T,
        outer_final,
        proj_out,
        final_out,
        proj_in,
        final_in,
    )


def any_shards(edge_embedding, alignment_embedding, tensor_flank_matrix, *others):
    groups = lax.axis_size("dap")
    rows, residues, width = edge_embedding.shape
    depth, _, features = alignment_embedding.shape
    hidden = tensor_flank_matrix.shape[1] // 2
    fits = (
        width == LANES
        and others[2].shape[0] == width
        and width % (groups * SUB) == 0
        and residues <= LANES
        and residues % SUB == 0
        and (rows * hidden // 2) % 16 == 0
        and (rows * width // groups) % 16 == 0
        and 2 * depth == LANES
        and hidden == 32
        and features % LANES == 0
        and (features // LANES) * (hidden // SUB) <= groups
        and hidden * hidden % (groups * SUB) == 0
    )
    program = kernel_shards if fits else shards
    return program(edge_embedding, alignment_embedding, tensor_flank_matrix, *others)


def solution(mesh):
    placed = (
        P(("dp", "dap"), None, None),
        P("dp", "dap", None),
        P(),
        P(),
        P(),
        P(),
        P(),
        P(),
        P(("dp", "dap"), None, None),
    )
    return jax.shard_map(
        any_shards,
        mesh=mesh,
        in_specs=placed,
        out_specs=(
            P(("dp", "dap"), None, None),
            P(("dp", "dap"), None, None),
            P("dp", "dap", None),
            P("dp", None),
            P("dp", None),
            P("dp", None),
            P("dp", None),
            P("dp", None),
            P("dp", None),
        ),
        check_vma=False,
    )
```
